32 devices in a mesh: rep: 8 (over z, core), tp: 4 (over y, x).
Axes of the slice: x: 2, y: 2, z: 4, core: 2. Of those that a mesh axis runs over, the one named last changes fastest.
Arguments:
- hidden_state: bfloat16 [32, 3584], P('rep'), may hold values from -6 to 6
- lengths: int32 [32], P('rep'), may hold values from 1 to 2048, as said below
- old_qkv: bfloat16 [3584, 4608], P(None, 'tp'), may hold values from -0.09375 to 0.09375
- old_out: bfloat16 [3584, 3584], P(None, 'tp'), may hold values from -0.09375 to 0.09375
- cache_keys: bfloat16 [32, 2048, 512], P('rep', 'tp'), may hold values from -64 to 64
- cache_values: bfloat16 [32, 2048, 512], P('rep', 'tp'), may hold values from -6 to 6
- new_qkv: bfloat16 [3584, 4608], P(('rep', 'tp')), may hold values from -0.09375 to 0.09375
- new_out: bfloat16 [3584, 3584], P(('rep', 'tp')), may hold values from -0.09375 to 0.09375
Outputs:
- decoded: bfloat16 [32, 3584], P('rep', 'tp')
- resharded_qkv: bfloat16 [3584, 4608], P(None, 'tp')
- resharded_out: bfloat16 [3584, 3584], P(None, 'tp')
The draws below stay inside these ranges and needn't reach their ends.
Inputs may be any that keep to these rules, and one draw needn't show every extreme that they name: Every sequence has 1 to 2048 cached tokens, held in positions 0 to lengths - 1; in every draw some sequence fills its cache.
All inputs are finite; a program needn't handle non-finite values.
Results may differ from the reference program's by a relative error of at most 0.012.
Values may be sent and summed in bfloat16 or wider, within the bound.
A program may use at most 128 MiB of HBM per device.

```python
import jax
import jax.numpy as jnp
from jax import lax

D = 3584
HQ = 28
KVH = 4
HD = 128
SEQS = 32
CACHE_LEN = 2048
COLS = 4608


def draw_lengths(key, part):
    drawn = jax.random.randint(key, (SEQS,), 1, CACHE_LEN + 1)
    chosen = jax.random.randint(jax.random.fold_in(key, 7), (), 0, SEQS)
    return jnp.where(jnp.arange(SEQS) == chosen, CACHE_LEN, drawn).astype(jnp.int32)


def draw_cache_keys(key, part):
    drawn = jax.random.normal(key, (SEQS, CACHE_LEN, KVH * HD), jnp.float32)
    return jnp.clip(drawn, -64.0, 64.0).astype(jnp.bfloat16)


def levels(rng, dims, pieces, least, largest):
    level = 1.0
    for axis_at, shards_of in pieces:
        steps = jax.random.uniform(jax.random.fold_in(jax.random.fold_in(rng, 6), axis_at), (shards_of,), jnp.float32, least / len(pieces), largest / len(pieces))
        level = level * jnp.repeat(jnp.exp(steps), dims[axis_at] // shards_of).reshape((-1,) + (1,) * (len(dims) - 1 - axis_at))
    return level


def bell_draw(stream_key, shape, deviation, bound, cuts=(), kind=jnp.bfloat16):
    values = deviation * jax.random.normal(stream_key, shape, jnp.float32)
    if cuts:
        values = values * levels(stream_key, shape, cuts, -0.22, 0.18)
    return jnp.clip(values, -bound, bound).astype(kind)


def setup_inputs(seed: int = 0) -> dict:
    splits = jax.random.split(jax.random.key(seed), 9)
    return {
        "hidden_state": bell_draw(splits[0], (SEQS, D), 1.0, 6.0, ((0, 8),)),
        "lengths": draw_lengths(jax.random.fold_in(splits[8], 71), 0),
        "old_qkv": bell_draw(splits[2], (D, COLS), D ** -0.5, 0.09375, ((1, 4),)),
        "old_out": bell_draw(splits[3], (HQ * HD, D), (HQ * HD) ** -0.5, 0.09375, ((1, 4),)),
        "cache_keys": draw_cache_keys(jax.random.fold_in(splits[8], 71), 0),
        "cache_values": bell_draw(splits[5], (SEQS, CACHE_LEN, KVH * HD), 1.0, 6.0, ((0, 8), (1, 4))),
        "new_qkv": bell_draw(splits[6], (D, COLS), D ** -0.5, 0.09375, ((0, 32),)),
        "new_out": bell_draw(splits[7], (HQ * HD, D), (HQ * HD) ** -0.5, 0.09375, ((0, 32),)),
    }


ROPE_BASE = 1000000.0

def rotate(vectors, positions):
    half_dim = vectors.shape[-1] // 2
    frequency = ROPE_BASE ** (-2.0 * jnp.arange(half_dim, dtype=jnp.float32) / (2 * half_dim))
    angles = positions.astype(jnp.float32)[:, None, None] * frequency
    first_half = vectors[..., :half_dim]
    second_half = vectors[..., half_dim:]
    return jnp.concatenate([first_half * jnp.cos(angles) - second_half * jnp.sin(angles), second_half * jnp.cos(angles) + first_half * jnp.sin(angles)], axis=-1)

def reference(hidden_state, lengths, old_qkv, old_out, cache_keys, cache_values, new_qkv, new_out):
    joined = jnp.dot(hidden_state, old_qkv, preferred_element_type=jnp.float32).astype(jnp.bfloat16)
    q_width = HQ * HD
    k_width = KVH * HD
    queries = rotate(joined[:, :q_width].astype(jnp.float32).reshape(SEQS, HQ, HD), lengths).astype(jnp.bfloat16)
    own_keys = rotate(joined[:, q_width:q_width + k_width].astype(jnp.float32).reshape(SEQS, KVH, HD), lengths).astype(jnp.bfloat16)
    own_values = joined[:, q_width + k_width:].reshape(SEQS, KVH, HD)
    group_size = HQ // KVH
    inv_root = 1.0 / jnp.sqrt(jnp.float32(HD))

    def attend(per_sequence):
        query_row, own_key, own_value, length, seq_keys, seq_values = per_sequence
        grouped = query_row.reshape(KVH, group_size, HD).astype(jnp.float32)
        key_blocks = seq_keys.reshape(CACHE_LEN, KVH, HD).astype(jnp.float32)
        value_blocks = seq_values.reshape(CACHE_LEN, KVH, HD).astype(jnp.float32)
        scores = jnp.einsum('kgd,tkd->kgt', grouped, key_blocks) * inv_root
        live_mask = jnp.arange(CACHE_LEN, dtype=jnp.int32) < length
        scores = jnp.where(live_mask, scores, jnp.float32(-1e+30))
        own_score = lax.optimization_barrier(jnp.sum(grouped * own_key.astype(jnp.float32)[:, None, :], axis=-1)) * inv_root
        top_score = jnp.maximum(lax.optimization_barrier(jnp.max(scores, axis=-1)), own_score)
        weights = jnp.where(live_mask, jnp.exp(scores - top_score[..., None]), jnp.float32(0.0)).astype(jnp.bfloat16)
        own_weight = lax.optimization_barrier(jnp.exp(own_score - top_score).astype(jnp.bfloat16)).astype(jnp.float32)
        numerator = jnp.einsum('kgt,tkd->kgd', weights.astype(jnp.float32), value_blocks)
        numerator = numerator + own_weight[..., None] * own_value.astype(jnp.float32)[:, None, :]
        denominator = lax.optimization_barrier(jnp.sum(weights.astype(jnp.float32), axis=-1)) + own_weight
        return (numerator / denominator[..., None]).reshape(HQ * HD).astype(jnp.bfloat16)
    attended = lax.map(attend, (queries, own_keys, own_values, lengths, cache_keys, cache_values))
    decoded = jnp.dot(attended, old_out, preferred_element_type=jnp.float32).astype(jnp.bfloat16)
    return (decoded, new_qkv, new_out)
```

```python
import functools

import jax
import jax.numpy as jnp
import numpy as np
from jax import lax
from jax.experimental import pallas as pl
from jax.experimental.pallas import tpu as pltpu
from jax.sharding import PartitionSpec as P

HQ = 28
KVH = 4
HD = 128
PAD = 8
CUTS = 8
LAST = 3
VMEM_BYTES = 67043328
SLACK = 600000
MESH = pl.DeviceIdType.MESH


ROPE_BASE = 1000000.0


def rotate(vectors, positions):
    half_dim = vectors.shape[-1] // 2
    frequency = ROPE_BASE ** (-2.0 * jnp.arange(half_dim, dtype=jnp.float32) / (2 * half_dim))
    angles = positions.astype(jnp.float32)[:, None, None] * frequency
    first_half = vectors[..., :half_dim]
    second_half = vectors[..., half_dim:]
    return jnp.concatenate(
        [
            first_half * jnp.cos(angles) - second_half * jnp.sin(angles),
            second_half * jnp.cos(angles) + first_half * jnp.sin(angles),
        ],
        axis=-1,
    )


def per_device(hidden_state, lengths, old_qkv, old_out, cache_keys, cache_values):
    seq_count = hidden_state.shape[0]
    local_joined = jnp.dot(hidden_state, old_qkv, preferred_element_type=jnp.float32).astype(
        jnp.bfloat16
    )
    joined_rows = lax.all_gather(local_joined, "tp", axis=1, tiled=True)
    q_width = HQ * HD
    k_width = KVH * HD
    group_size = HQ // KVH
    queries = rotate(
        joined_rows[:, :q_width].astype(jnp.float32).reshape(seq_count, HQ, HD), lengths
    ).astype(jnp.bfloat16)
    own_keys = rotate(
        joined_rows[:, q_width : q_width + k_width].astype(jnp.float32).reshape(seq_count, KVH, HD),
        lengths,
    ).astype(jnp.bfloat16)
    own_values = joined_rows[:, q_width + k_width :].reshape(seq_count, KVH, HD)
    inv_root = 1.0 / jnp.sqrt(jnp.float32(HD))
    cache_rows = cache_keys.shape[1]
    grouped = queries.reshape(seq_count, KVH, group_size, HD)
    key_blocks = cache_keys.reshape(seq_count, cache_rows, KVH, HD)
    value_blocks = cache_values.reshape(seq_count, cache_rows, KVH, HD)
    scores = (
        jnp.einsum("skgd,stkd->skgt", grouped, key_blocks, preferred_element_type=jnp.float32)
        * inv_root
    )
    positions = lax.axis_index("tp") * cache_rows + jnp.arange(cache_rows, dtype=jnp.int32)
    live_mask = (positions[None, :] < lengths[:, None])[:, None, None, :]
    scores = jnp.where(live_mask, scores, jnp.float32(-1e30))
    own_score = (
        jnp.sum(grouped.astype(jnp.float32) * own_keys.astype(jnp.float32)[:, :, None, :], axis=-1)
        * inv_root
    )
    local_top = jnp.maximum(jnp.max(scores, axis=-1), own_score)
    top_score = lax.pmax(local_top, "tp")
    weights = jnp.where(live_mask, jnp.exp(scores - top_score[..., None]), jnp.float32(0.0)).astype(
        jnp.bfloat16
    )
    numer_part = jnp.einsum(
        "skgt,stkd->skgd", weights, value_blocks, preferred_element_type=jnp.float32
    )
    denom_part = jnp.sum(weights.astype(jnp.float32), axis=-1)
    numerator, denominator = lax.psum((numer_part, denom_part), "tp")
    own_weight = lax.optimization_barrier(
        jnp.exp(own_score - top_score).astype(jnp.bfloat16)
    ).astype(jnp.float32)
    numerator = numerator + own_weight[..., None] * own_values.astype(jnp.float32)[:, :, None, :]
    denominator = denominator + own_weight
    attended = (numerator / denominator[..., None]).reshape(seq_count, q_width).astype(jnp.bfloat16)
    decoded = jnp.dot(attended, old_out, preferred_element_type=jnp.float32).astype(jnp.bfloat16)
    return decoded


def native_move(new_qkv, new_out):
    def move(block):
        piece = lax.all_to_all(block, "tp", split_axis=1, concat_axis=0, tiled=True)
        return lax.all_gather(piece, "rep", axis=0, tiled=True)

    return move(new_qkv), move(new_out)


def flip(index, bits, size):
    out = index
    bit = 1
    while bit < size:
        if (bits // bit) % 2:
            out = out + bit - 2 * bit * ((index // bit) % 2)
        bit *= 2
    return out


def step_kernel(
    planes, tps,
    hidden_in, lengths_in, frequency_in, old_qkv, old_out, keys, values, new_qkv, new_out,
    decoded, qkv_full, out_full,
    a_send, a_recv, z_send, z_recv, z_last, s_send, s_recv, s_last, own_sem, load_sem, small_sem,
    w_qkv, w_out, k_held, v_held, joined, rotated, own_score, own_value, parts, attended,
    cosine, sine, hidden, frequency, lengths,
):
    rep, tp = lax.axis_index("rep"), lax.axis_index("tp")
    plane, core = rep // 2, rep % 2
    rows = new_qkv.shape[0]
    blocks, fulls = (new_qkv, new_out), (qkv_full, out_full)
    widths = (qkv_full.shape[1], out_full.shape[1])
    up = (jnp.minimum(plane + 1, planes - 1) * 2 + core, tp)
    down = (jnp.maximum(plane - 1, 0) * 2 + core, tp)
    twin = (plane * 2 + 1 - core, tp)
    peers = [(rep, flip(tp, k, tps)) for k in range(1, tps)]
    near = [k for k in range(1, tps) if k & (k - 1) == 0]
    far = [k for k in range(1, tps) if k & (k - 1)]
    can_up, can_down = plane < planes - 1, plane > 0

    barrier = pltpu.get_barrier_semaphore()
    for device in [twin] + [peers[k - 1] for k in near]:
        pl.semaphore_signal(barrier, inc=1, device_id=device, device_id_type=MESH)

    @pl.when(can_up)
    def _():
        pl.semaphore_signal(barrier, inc=1, device_id=up, device_id_type=MESH)

    @pl.when(can_down)
    def _():
        pl.semaphore_signal(barrier, inc=1, device_id=down, device_id_type=MESH)

    small = [
        pltpu.make_async_copy(source, target, load_sem.at[4 + i])
        for i, (source, target) in enumerate(
            ((hidden_in, hidden), (frequency_in, frequency), (lengths_in, lengths))
        )
    ]
    for copy in small:
        copy.start()

    @pl.when(can_up & can_down)
    def _():
        pl.semaphore_wait(barrier, len(near) + 3)

    @pl.when(jnp.logical_not(can_up & can_down))
    def _():
        pl.semaphore_wait(barrier, len(near) + 2)

    def remote(source, target, send, recv, device):
        return pltpu.make_async_remote_copy(
            src_ref=source, dst_ref=target, send_sem=send, recv_sem=recv,
            device_id=device, device_id_type=MESH,
        )

    def sent(ref, sem):
        remote(ref, ref, sem, sem, twin).wait_send()

    def landed(ref, sem):
        remote(ref, ref, sem, sem, twin).wait_recv()

    half = tps // 2

    def at_rows(source_plane, source_core, first, count, w):
        start = ((source_plane * 2 + source_core) * tps) * rows + first
        return fulls[w].at[pl.ds(pl.multiple_of(start, 16), count)]

    def piece_rows(source_plane, source_core, k, w):
        return at_rows(source_plane, source_core, flip(tp, k, tps) * rows, rows, w)

    def pair_first(h):
        return (flip(tp, 2 * h, tps) // 2) * 2 * rows

    def chunks(last):
        cuts = [(h, w, 0, 2 * rows, None) for h in range(half) for w in range(2)]
        if last:
            h, w, _, count, _ = cuts.pop()
            step = max(16, count // LAST // 16 * 16)
            first = 0
            for i in range(LAST):
                size = step if i else count - (LAST - 1) * step
                cuts.append((h, w, first, size, i))
                first += size
        return cuts

    def chunk_rows(source_plane, source_core, chunk):
        h, w, first, count, _ = chunk
        return at_rows(source_plane, source_core, pair_first(h) + first, count, w)

    def chunk_sem(sems, lasts, source_plane, chunk):
        h, w, _, _, i = chunk
        return sems.at[source_plane, h, w] if i is None else lasts.at[i]

    def block_rows(source_plane, source_core, w):
        return at_rows(source_plane, source_core, 0, tps * rows, w)

    def column(w, t):
        return blocks[w].at[:, pl.ds(pl.multiple_of(t * widths[w], 128), widths[w])]

    def in_plane(k, w):
        remote(
            column(w, flip(tp, k, tps)), piece_rows(plane, core, 0, w),
            a_send.at[w], a_recv.at[k, w], peers[k - 1],
        ).start()

    def own(k, w):
        target = piece_rows(plane, core, k, w)
        source = column(w, tp) if k == 0 else target
        h = k // 2

        @pl.when(can_up)
        def _():
            remote(
                source, target, z_send.at[plane, w], z_recv.at[plane, h, w], up
            ).start()

        @pl.when(can_down)
        def _():
            remote(
                source, target, z_send.at[plane + 1, w], z_recv.at[plane, h, w], down
            ).start()

        remote(source, target, s_send.at[plane, w], s_recv.at[plane, h, w], twin).start()

    def take(source_plane, chunk, forward, slot, onward):
        target = chunk_rows(source_plane, core, chunk)
        landed(target, chunk_sem(z_recv, z_last, source_plane, chunk))
        w = chunk[1]
        if forward is not None:
            can, device = forward

            @pl.when(can)
            def _():
                for part in onward:
                    ref = chunk_rows(source_plane, core, part)
                    remote(
                        ref, ref, z_send.at[slot, w],
                        chunk_sem(z_recv, z_last, source_plane, part), device,
                    ).start()

        remote(
            target, target, s_send.at[source_plane, w],
            chunk_sem(s_recv, s_last, source_plane, chunk), twin,
        ).start()

    def relay(d):
        cuts = chunks(d == planes - 1)
        ahead = chunks(d == planes - 2)
        for chunk in cuts:
            onward = [part for part in ahead if part[:2] == chunk[:2]]
            below = (can_up, up) if d < planes - 1 else None
            above = (can_down, down) if d < planes - 1 else None

            @pl.when(plane >= d)
            def _():
                take(plane - d, chunk, below, plane - d, onward)

            @pl.when(plane + d < planes)
            def _():
                take(plane + d, chunk, above, plane + d + 1, onward)

    for w in range(2):
        own(0, w)
    for k in near:
        for w in range(2):
            in_plane(k, w)
    locals_ = [
        pltpu.make_async_copy(column(w, tp), piece_rows(plane, core, 0, w), own_sem.at[w])
        for w in range(2)
    ]
    loads = [
        pltpu.make_async_copy(source, target, load_sem.at[i])
        for i, (source, target) in enumerate(
            ((old_qkv, w_qkv), (keys, k_held), (values, v_held), (old_out, w_out))
        )
    ]
    for copy in locals_ + loads:
        copy.start()
    for k in near + far:
        for w in range(2):
            landed(piece_rows(plane, core, k, w), a_recv.at[k, w])
            own(k, w)
            if k == near[0] and w == 0:
                for j in far:
                    for v in range(2):
                        in_plane(j, v)

    for copy in small:
        copy.wait()
    seqs = hidden.shape[0]
    lane = lax.broadcasted_iota(jnp.int32, (1, HD), 1)
    for s in range(seqs):
        angles = lengths[s].astype(jnp.float32) * frequency[...]
        cosine[s : s + 1, :] = jnp.cos(angles)
        sine[s : s + 1, :] = jnp.where(lane < HD // 2, -jnp.sin(angles), jnp.sin(angles))
    tile = 128
    loads[0].wait()

    @pl.loop(0, w_qkv.shape[1] // tile)
    def _(i):
        at = pl.ds(pl.multiple_of(i * tile, tile), tile)
        joined[tp, :, at] = jnp.dot(
            hidden[...], w_qkv[:, at], preferred_element_type=jnp.float32
        ).astype(joined.dtype)

    def send_all(ref, send, recv):
        for k in range(1, tps):
            remote(ref.at[tp], ref.at[tp], send, recv, peers[k - 1]).start()

    send_all(joined, small_sem.at[0], small_sem.at[1])

    relay(1)

    landed(joined.at[pl.ds(0, tps - 1)], small_sem.at[1])
    for copy in loads[1:]:
        copy.wait()

    group = HQ // KVH
    positions = k_held.shape[1]
    per_slot = joined.shape[2] // HD
    inv_root = 1.0 / jnp.sqrt(jnp.float32(HD))

    def head(j):
        at = (j % per_slot) * HD
        return joined[j // per_slot, :, at : at + HD].astype(jnp.float32)

    def turn(v):
        swapped = jnp.concatenate([v[:, HD // 2 :], v[:, : HD // 2]], axis=1)
        return (v * cosine[...] + swapped * sine[...]).astype(jnp.bfloat16).astype(jnp.float32)

    rotated[...] = jnp.zeros_like(rotated)
    own_score[...] = jnp.zeros_like(own_score)
    own_value[...] = jnp.zeros_like(own_value)
    for kv in range(KVH):
        own_key = turn(head(HQ + kv))
        new_value = head(HQ + KVH + kv)
        for g in range(group):
            query = turn(head(kv * group + g))
            rotated[:, kv * PAD + g, :] = query
            score = jnp.sum(query * own_key, axis=1, keepdims=True) * inv_root
            own_score[:, kv * PAD + g, :] = jnp.broadcast_to(score, (seqs, HD))
            own_value[:, kv * PAD + g, :] = new_value

    @pl.loop(0, seqs)
    def _(s):
        place = lax.broadcasted_iota(jnp.int32, (1, positions), 1) + tp * positions
        is_live = place < lengths[s]
        for kv in range(KVH):
            at = slice(kv * HD, (kv + 1) * HD)
            lanes = slice(kv * PAD, (kv + 1) * PAD)
            query = rotated[s, lanes, :].astype(jnp.bfloat16)
            scores = lax.dot_general(
                query, k_held[s, :, at], (((1,), (1,)), ((), ())),
                preferred_element_type=jnp.float32,
            ) * inv_root
            scores = jnp.where(is_live, scores, jnp.float32(-1e30))
            top = jnp.max(scores, axis=1, keepdims=True)
            weights = jnp.where(is_live, jnp.exp(scores - top), 0.0).astype(jnp.bfloat16)
            total = jnp.sum(weights.astype(jnp.float32), axis=1, keepdims=True)
            parts[tp, 0, s, lanes, :] = jnp.dot(
                weights, v_held[s, :, at], preferred_element_type=jnp.float32
            )
            parts[tp, 1, s, lanes, :] = jnp.broadcast_to(top, (PAD, HD))
            parts[tp, 2, s, lanes, :] = jnp.broadcast_to(total, (PAD, HD))

    send_all(parts, small_sem.at[2], small_sem.at[3])

    for d in range(2, planes - 1):
        relay(d)

    landed(parts.at[pl.ds(0, tps - 1)], small_sem.at[3])

    @pl.loop(0, seqs)
    def _(s):
        mine = own_score[s]
        top = mine
        for t in range(tps):
            top = jnp.maximum(top, parts[t, 1, s])
        mine = jnp.exp(mine - top).astype(jnp.bfloat16).astype(jnp.float32)
        numerator, denominator = mine * own_value[s], mine
        for t in range(tps):
            scale = jnp.exp(parts[t, 1, s] - top)
            numerator = numerator + parts[t, 0, s] * scale
            denominator = denominator + parts[t, 2, s] * scale
        rotated[s] = numerator / denominator

    for j in range(HQ):
        row = (j // group) * PAD + j % group
        attended[:, j * HD : (j + 1) * HD] = rotated[:, row, :].astype(attended.dtype)

    @pl.loop(0, w_out.shape[1] // tile)
    def _(i):
        at = pl.ds(pl.multiple_of(i * tile, tile), tile)
        decoded[:, at] = jnp.dot(
            attended[...], w_out[:, at], preferred_element_type=jnp.float32
        ).astype(decoded.dtype)

    def from_twin(source_plane, last):
        for chunk in chunks(last):
            landed(
                chunk_rows(source_plane, 1 - core, chunk),
                chunk_sem(s_recv, s_last, source_plane, chunk),
            )

    def to_twin(source_plane):
        for w in range(2):
            sent(block_rows(source_plane, core, w), s_send.at[source_plane, w])

    def to_next(d):
        for w in range(2):

            @pl.when((plane >= d) & can_up)
            def _():
                sent(block_rows(plane - d, core, w), z_send.at[plane - d, w])

            @pl.when((plane + d < planes) & can_down)
            def _():
                sent(block_rows(plane + d, core, w), z_send.at[plane + d + 1, w])

    for w in range(2):
        sent(fulls[w].at[pl.ds(0, (tps - 1) * rows)], a_send.at[w])
    sent(joined.at[pl.ds(0, tps - 1)], small_sem.at[0])
    sent(parts.at[pl.ds(0, tps - 1)], small_sem.at[2])
    for copy in locals_:
        copy.wait()
    for d in range(planes - 1):

        @pl.when(plane >= d)
        def _():
            from_twin(plane - d, False)
            to_twin(plane - d)

        if d:

            @pl.when(plane + d < planes)
            def _():
                from_twin(plane + d, False)
                to_twin(plane + d)

    to_next(0)
    relay(planes - 1)
    d = planes - 1

    @pl.when(plane >= d)
    def _():
        from_twin(plane - d, True)
        to_twin(plane - d)

    @pl.when(plane + d < planes)
    def _():
        from_twin(plane + d, True)
        to_twin(plane + d)

    for d in range(1, planes - 1):
        to_next(d)


def flush_kernel(decoded, qkv, out, decoded_to, qkv_to, out_to, sems):
    copies = [pltpu.make_async_copy(decoded, decoded_to, sems.at[0])]
    for source, target in ((qkv, qkv_to), (out, out_to)):
        rows = source.shape[0] // CUTS
        for i in range(CUTS):
            at = pl.ds(i * rows, rows)
            copies.append(
                pltpu.make_async_copy(source.at[at], target.at[at], sems.at[len(copies)])
            )
    for copy in copies:
        copy.start()
    for copy in copies:
        copy.wait()


def flush(*arrays):
    return pl.pallas_call(
        flush_kernel,
        out_shape=[jax.ShapeDtypeStruct(x.shape, x.dtype) for x in arrays],
        in_specs=[pl.BlockSpec(memory_space=pltpu.VMEM)] * 3,
        out_specs=[pl.BlockSpec(memory_space=pltpu.HBM)] * 3,
        scratch_shapes=[pltpu.SemaphoreType.DMA((2 * CUTS + 1,))],
        compiler_params=pltpu.CompilerParams(vmem_limit_bytes=2**20),
    )(*arrays)


def fused(mesh, hidden, lengths, old_qkv, old_out, keys, values, new_qkv, new_out):
    reps, tps = mesh.shape["rep"], mesh.shape["tp"]
    planes = reps // 2
    seqs = keys.shape[0]
    rows = new_qkv.shape[0]
    widths = (new_qkv.shape[1] // tps, new_out.shape[1] // tps)
    half = HD // 2
    frequency = ROPE_BASE ** (-2.0 * np.arange(half) / (2 * half))
    frequency = jnp.asarray(np.concatenate([frequency, frequency])[None], jnp.float32)

    sem = pltpu.SemaphoreType.DMA
    whole, anywhere = pl.BlockSpec(memory_space=pltpu.VMEM), pl.BlockSpec(memory_space=pl.ANY)
    in_hbm = pl.BlockSpec(memory_space=pltpu.HBM)
    f32, bf16 = jnp.float32, jnp.bfloat16
    padded = KVH * PAD
    landed = 2 * rows * reps * tps * sum(widths)
    half = tps // 2
    scratch = [sem((2,)), sem((tps, 2)), sem((planes + 1, 2)), sem((planes, half, 2)), sem((LAST,))]
    scratch += [sem((planes, 2)), sem((planes, half, 2)), sem((LAST,))]
    scratch += [sem((2,)), sem((7,)), sem((4,))]
    scratch += [pltpu.VMEM(x.shape, x.dtype) for x in (old_qkv, old_out, keys, values)]
    scratch += [
        pltpu.VMEM((tps, seqs, widths[0]), bf16),
        pltpu.VMEM((seqs, padded, HD), f32),
        pltpu.VMEM((seqs, padded, HD), f32),
        pltpu.VMEM((seqs, padded, HD), f32),
        pltpu.VMEM((tps, 3, seqs, padded, HD), f32),
        pltpu.VMEM((seqs, HQ * HD), bf16),
        pltpu.VMEM((seqs, HD), f32),
        pltpu.VMEM((seqs, HD), f32),
        pltpu.VMEM(hidden.shape, hidden.dtype),
        pltpu.VMEM(frequency.shape, frequency.dtype),
        pltpu.SMEM(lengths.shape, lengths.dtype),
    ]
    return pl.pallas_call(
        functools.partial(step_kernel, planes, tps),
        out_shape=[pltpu.VMEM((seqs, widths[1]), bf16)]
        + [pltpu.VMEM((rows * reps * tps, width), bf16) for width in widths],
        in_specs=[in_hbm] * 9,
        out_specs=[whole] + [anywhere] * 2,
        scratch_shapes=scratch,
        compiler_params=pltpu.CompilerParams(
            collective_id=0, has_side_effects=True, vmem_limit_bytes=VMEM_BYTES - landed - SLACK
        ),
    )(hidden, lengths, frequency, old_qkv, old_out, keys, values, new_qkv, new_out)


def solution(mesh):
    in_specs = (
        P("rep", None),
        P("rep"),
        P(None, "tp"),
        P(None, "tp"),
        P("rep", "tp", None),
        P("rep", "tp", None),
        P(("rep", "tp"), None),
        P(("rep", "tp"), None),
    )
    out_specs = (P("rep", "tp"), P(None, "tp"), P(None, "tp"))

    def step(*args):
        reps, tps = mesh.shape["rep"], mesh.shape["tp"]
        widths = [x.shape[1] // tps for x in args[6:]]
        tiled = args[6].shape[0] % 16 == 0 and all(width % 128 == 0 for width in widths)
        if reps % 4 or reps < 6 or tps != 4 or not tiled:
            return (per_device(*args[:6]), *native_move(*args[6:]))
        return tuple(flush(*fused(mesh, *args)))

    return jax.shard_map(
        step, mesh=mesh, in_specs=in_specs, out_specs=out_specs, check_vma=False
    )
```

```python
import functools

import jax
import jax.numpy as jnp
import numpy as np
from jax import lax
from jax.experimental import pallas as pl
from jax.experimental.pallas import tpu as pltpu
from jax.sharding import PartitionSpec as P

HQ = 28
KVH = 4
HD = 128
PAD = 8
CUTS = 28
TAIL = 4
VMEM_BYTES = 67043328
SLACK = 600000
MESH = pl.DeviceIdType.MESH


ROPE_BASE = 1000000.0


def rotate(vectors, positions):
    half_dim = vectors.shape[-1] // 2
    frequency = ROPE_BASE ** (-2.0 * jnp.arange(half_dim, dtype=jnp.float32) / (2 * half_dim))
    angles = positions.astype(jnp.float32)[:, None, None] * frequency
    first_half = vectors[..., :half_dim]
    second_half = vectors[..., half_dim:]
    return jnp.concatenate(
        [
            first_half * jnp.cos(angles) - second_half * jnp.sin(angles),
            second_half * jnp.cos(angles) + first_half * jnp.sin(angles),
        ],
        axis=-1,
    )


def per_device(hidden_state, lengths, old_qkv, old_out, cache_keys, cache_values):
    seq_count = hidden_state.shape[0]
    local_joined = jnp.dot(hidden_state, old_qkv, preferred_element_type=jnp.float32).astype(
        jnp.bfloat16
    )
    joined_rows = lax.all_gather(local_joined, "tp", axis=1, tiled=True)
    q_width = HQ * HD
    k_width = KVH * HD
    group_size = HQ // KVH
    queries = rotate(
        joined_rows[:, :q_width].astype(jnp.float32).reshape(seq_count, HQ, HD), lengths
    ).astype(jnp.bfloat16)
    own_keys = rotate(
        joined_rows[:, q_width : q_width + k_width].astype(jnp.float32).reshape(seq_count, KVH, HD),
        lengths,
    ).astype(jnp.bfloat16)
    own_values = joined_rows[:, q_width + k_width :].reshape(seq_count, KVH, HD)
    inv_root = 1.0 / jnp.sqrt(jnp.float32(HD))
    cache_rows = cache_keys.shape[1]
    grouped = queries.reshape(seq_count, KVH, group_size, HD)
    key_blocks = cache_keys.reshape(seq_count, cache_rows, KVH, HD)
    value_blocks = cache_values.reshape(seq_count, cache_rows, KVH, HD)
    scores = (
        jnp.einsum("skgd,stkd->skgt", grouped, key_blocks, preferred_element_type=jnp.float32)
        * inv_root
    )
    positions = lax.axis_index("tp") * cache_rows + jnp.arange(cache_rows, dtype=jnp.int32)
    live_mask = (positions[None, :] < lengths[:, None])[:, None, None, :]
    scores = jnp.where(live_mask, scores, jnp.float32(-1e30))
    own_score = (
        jnp.sum(grouped.astype(jnp.float32) * own_keys.astype(jnp.float32)[:, :, None, :], axis=-1)
        * inv_root
    )
    local_top = jnp.maximum(jnp.max(scores, axis=-1), own_score)
    top_score = lax.pmax(local_top, "tp")
    weights = jnp.where(live_mask, jnp.exp(scores - top_score[..., None]), jnp.float32(0.0)).astype(
        jnp.bfloat16
    )
    numer_part = jnp.einsum(
        "skgt,stkd->skgd", weights, value_blocks, preferred_element_type=jnp.float32
    )
    denom_part = jnp.sum(weights.astype(jnp.float32), axis=-1)
    numerator, denominator = lax.psum((numer_part, denom_part), "tp")
    own_weight = lax.optimization_barrier(
        jnp.exp(own_score - top_score).astype(jnp.bfloat16)
    ).astype(jnp.float32)
    numerator = numerator + own_weight[..., None] * own_values.astype(jnp.float32)[:, :, None, :]
    denominator = denominator + own_weight
    attended = (numerator / denominator[..., None]).reshape(seq_count, q_width).astype(jnp.bfloat16)
    decoded = jnp.dot(attended, old_out, preferred_element_type=jnp.float32).astype(jnp.bfloat16)
    return decoded


def native_move(new_qkv, new_out):
    def move(block):
        piece = lax.all_to_all(block, "tp", split_axis=1, concat_axis=0, tiled=True)
        return lax.all_gather(piece, "rep", axis=0, tiled=True)

    return move(new_qkv), move(new_out)


def flip(index, bits, size):
    out = index
    bit = 1
    while bit < size:
        if (bits // bit) % 2:
            out = out + bit - 2 * bit * ((index // bit) % 2)
        bit *= 2
    return out


def step_kernel(
    planes, tps,
    hidden_in, lengths_in, frequency_in, old_qkv, old_out, keys, values, new_qkv, new_out,
    decoded, qkv_full, out_full,
    a_send, a_recv, z_send, z_recv, z_last, s_send, s_recv, t_send, t_recv, own_sem,
    load_sem, small_sem, met,
    stage,
    w_qkv, w_out, k_held, v_held, joined, rotated, own_score, own_value, parts, attended,
    cosine, sine, hidden, frequency, lengths,
):
    rep, tp = lax.axis_index("rep"), lax.axis_index("tp")
    plane, core = rep // 2, rep % 2
    rows = new_qkv.shape[0]
    fulls = (qkv_full, out_full)
    widths = (qkv_full.shape[1], out_full.shape[1])
    bases = (0, new_qkv.shape[1])
    up = (jnp.minimum(plane + 1, planes - 1) * 2 + core, tp)
    down = (jnp.maximum(plane - 1, 0) * 2 + core, tp)
    twin = (plane * 2 + 1 - core, tp)
    peers = [(rep, flip(tp, k, tps)) for k in range(1, tps)]
    near = [k for k in range(1, tps) if k & (k - 1) == 0]
    far = [k for k in range(1, tps) if k & (k - 1)]
    can_up, can_down = plane < planes - 1, plane > 0

    barrier = pltpu.get_barrier_semaphore()
    beside = [twin] + [peers[k - 1] for k in near]

    def tell(semaphore, device):
        pl.semaphore_signal(semaphore, inc=1, device_id=device, device_id_type=MESH)

    @pl.when(can_up)
    def _():
        tell(barrier, up)

    @pl.when(can_down & (plane != 2))
    def _():
        tell(barrier, down)

    @pl.when(plane != 1)
    def _():
        for device in beside:
            tell(barrier, device)

    half = tps // 2

    def at_rows(source_plane, source_core, first, count, w):
        start = ((source_plane * 2 + source_core) * tps) * rows + first
        return fulls[w].at[pl.ds(pl.multiple_of(start, 16), count)]

    def piece_rows(source_plane, source_core, k, w):
        return at_rows(source_plane, source_core, flip(tp, k, tps) * rows, rows, w)

    mine = [
        pltpu.make_async_copy(
            source.at[:, pl.ds(pl.multiple_of(tp * widths[w], 128), widths[w])],
            piece_rows(plane, core, 0, w), own_sem.at[w],
        )
        for w, source in enumerate((new_qkv, new_out))
    ]
    staged = [
        pltpu.make_async_copy(
            source, stage.at[:, pl.ds(bases[w], source.shape[1])], own_sem.at[2 + w]
        )
        for w, source in enumerate((new_qkv, new_out))
    ]
    for copy in mine + staged:
        copy.start()
    small = [
        pltpu.make_async_copy(source, target, load_sem.at[4 + i])
        for i, (source, target) in enumerate(
            ((hidden_in, hidden), (frequency_in, frequency), (lengths_in, lengths))
        )
    ]

    @pl.when(plane == 1)
    def _():
        pl.semaphore_wait(barrier, 1)

    @pl.when((plane != 1) & can_up & can_down)
    def _():
        pl.semaphore_wait(barrier, len(beside) + 2)

    @pl.when(jnp.logical_not(can_up & can_down))
    def _():
        pl.semaphore_wait(barrier, len(beside) + 1)

    def remote(source, target, send, recv, device):
        return pltpu.make_async_remote_copy(
            src_ref=source, dst_ref=target, send_sem=send, recv_sem=recv,
            device_id=device, device_id_type=MESH,
        )

    def sent(ref, sem):
        remote(ref, ref, sem, sem, twin).wait_send()

    def landed(ref, sem):
        remote(ref, ref, sem, sem, twin).wait_recv()

    def pair_first(h):
        return (flip(tp, 2 * h, tps) // 2) * 2 * rows

    tail = TAIL * 16
    tails = [(1, first, count) for first, count in ((2 * rows - tail, tail - 16), (2 * rows - 16, 16))]
    tails = [(c, part) for part in tails for c in (1, 0)]

    def parts_of(h, last):
        if last and h == half - 1:
            return [(0, 0, 2 * rows, 0), (1, 0, 2 * rows - tail, 1)]
        return [(w, 0, 2 * rows, None) for w in range(2)]

    def part_rows(source_plane, source_core, h, part):
        w, first, count = part[:3]
        return at_rows(source_plane, source_core, pair_first(h) + first, count, w)

    def part_sem(source_plane, h, part):
        return z_recv.at[source_plane, h] if part[3] is None else z_last.at[part[3]]

    def bytes_of(parts):
        return stage.at[:, pl.ds(0, stage.shape[1] // tps * parts)]

    def out_rows(count):
        return out_full.at[pl.ds(0, count)]

    def block_bytes(last):
        if last:
            return out_rows(rows * tps * sum(widths) // widths[1] - tail)
        return stage

    def send_tails(source_plane, device):
        for i, (c, part) in enumerate(tails):
            ref = part_rows(source_plane, c, half - 1, part)
            remote(ref, ref, t_send.at[0], t_recv.at[i], device).start()

    def take_tails(source_plane):
        for i, (c, part) in enumerate(tails):
            ref = part_rows(source_plane, c, half - 1, part)
            landed(ref, t_recv.at[i])
            remote(ref, ref, t_send.at[1], t_recv.at[len(tails)], twin).start()

    def column(w, t):
        start = bases[w] + t * widths[w]
        return stage.at[:, pl.ds(pl.multiple_of(start, 128), widths[w])]

    def in_plane(k, w):
        remote(
            column(w, flip(tp, k, tps)), piece_rows(plane, core, 0, w),
            a_send.at[0], a_recv.at[k - 1, w], peers[k - 1],
        ).start()

    def own_up(k, w):
        ref = piece_rows(plane, core, k, w)

        @pl.when(can_up)
        def _():
            remote(ref, ref, z_send.at[plane], z_recv.at[plane, k // 2], up).start()

    def own_down(k, w):
        ref = piece_rows(plane, core, k, w)

        @pl.when(can_down)
        def _():
            remote(ref, ref, z_send.at[plane + 1], z_recv.at[plane, k // 2], down).start()

    def own_twin(k, w):
        ref = piece_rows(plane, core, k, w)
        remote(ref, ref, s_send.at[plane], s_recv.at[plane], twin).start()

    def take(source_plane, h, last, parts, forward, slot, onward):
        if last:
            (part,) = parts
            landed(part_rows(source_plane, core, h, part), part_sem(source_plane, h, part))
        else:
            landed(bytes_of(2), z_recv.at[source_plane, h])
        if forward is not None:
            can, device = forward

            @pl.when(can)
            def _():
                for part in onward:
                    ref = part_rows(source_plane, core, h, part)
                    remote(
                        ref, ref, z_send.at[slot], part_sem(source_plane, h, part), device
                    ).start()

        for part in parts:
            ref = part_rows(source_plane, core, h, part)
            remote(ref, ref, s_send.at[source_plane], s_recv.at[source_plane], twin).start()

    def relay(d):
        ends = d == planes - 1
        for h in range(half):
            cuts = parts_of(h, ends)
            onward = parts_of(h, d == planes - 2)
            single = ends and h == half - 1
            for parts in [[part] for part in cuts] if single else [cuts]:

                @pl.when(plane >= d)
                def _():
                    take(plane - d, h, single, parts, None if ends else (can_up, up), plane - d, onward)

                @pl.when(plane + d < planes)
                def _():
                    take(
                        plane + d, h, single, parts,
                        None if ends else (can_down, down), plane + d + 1, onward,
                    )

    def settle_twin(source_plane, last):
        landed(block_bytes(last), s_recv.at[source_plane])
        sent(block_bytes(last), s_send.at[source_plane])

    def settle_next(d):
        @pl.when((plane >= d) & can_up)
        def _():
            sent(block_bytes(d == planes - 2), z_send.at[plane - d])

        @pl.when((plane + d < planes) & can_down)
        def _():
            sent(block_bytes(d == planes - 2), z_send.at[plane + d + 1])

    def settle(d):
        @pl.when(plane >= d)
        def _():
            settle_twin(plane - d, d == planes - 1)

        if d:

            @pl.when(plane + d < planes)
            def _():
                settle_twin(plane + d, d == planes - 1)

    for w in range(2):
        mine[w].wait()
        own_down(0, w)

    def open_plane():
        for w in (1, 0):
            staged[w].wait()
            for k in near:
                in_plane(k, w)
        for w in range(2):
            own_twin(0, w)

    @pl.when(plane == 0)
    def _():
        for device in beside:
            tell(met.at[0], device)

    @pl.when(plane == 2)
    def _():
        tell(met.at[1], down)

    @pl.when(plane != 1)
    def _():
        for w in range(2):
            own_up(0, w)
        open_plane()

    @pl.when(plane == 0)
    def _():
        pl.semaphore_wait(met.at[0], len(beside))
        tell(met.at[2], up)

    @pl.when(plane == 1)
    def _():
        pl.semaphore_wait(met.at[2], 1)
        open_plane()
        pl.semaphore_wait(met.at[1], 1)
        for w in range(2):
            own_up(0, w)

    loads = [
        pltpu.make_async_copy(source, target, load_sem.at[i])
        for i, (source, target) in enumerate(
            ((old_qkv, w_qkv), (keys, k_held), (values, v_held), (old_out, w_out))
        )
    ]
    for copy in loads + small:
        copy.start()
    arrivals = [(k, w) for w in (1, 0) for k in near] + [(k, w) for k in far for w in (1, 0)]
    for k, w in arrivals:
        landed(piece_rows(plane, core, k, w), a_recv.at[k - 1, w])
        own_down(k, w)
        own_up(k, w)
        own_twin(k, w)
        if (k, w) == arrivals[0]:
            for j in far:
                for v in (1, 0):
                    in_plane(j, v)

    for copy in small:
        copy.wait()
    seqs = hidden.shape[0]
    lane = lax.broadcasted_iota(jnp.int32, (1, HD), 1)
    for s in range(seqs):
        angles = lengths[s].astype(jnp.float32) * frequency[...]
        cosine[s : s + 1, :] = jnp.cos(angles)
        sine[s : s + 1, :] = jnp.where(lane < HD // 2, -jnp.sin(angles), jnp.sin(angles))
    tile = 128
    loads[0].wait()

    @pl.loop(0, w_qkv.shape[1] // tile)
    def _(i):
        at = pl.ds(pl.multiple_of(i * tile, tile), tile)
        joined[tp, :, at] = jnp.dot(
            hidden[...], w_qkv[:, at], preferred_element_type=jnp.float32
        ).astype(joined.dtype)

    def send_all(ref, send, recv):
        for k in range(1, tps):
            remote(ref.at[tp], ref.at[tp], send, recv, peers[k - 1]).start()

    send_all(joined, small_sem.at[0], small_sem.at[1])

    relay(1)

    landed(joined.at[pl.ds(0, tps - 1)], small_sem.at[1])
    for copy in loads[1:]:
        copy.wait()

    group = HQ // KVH
    positions = k_held.shape[1]
    per_slot = joined.shape[2] // HD
    inv_root = 1.0 / jnp.sqrt(jnp.float32(HD))

    def head(j):
        at = (j % per_slot) * HD
        return joined[j // per_slot, :, at : at + HD].astype(jnp.float32)

    def turn(v):
        swapped = jnp.concatenate([v[:, HD // 2 :], v[:, : HD // 2]], axis=1)
        return (v * cosine[...] + swapped * sine[...]).astype(jnp.bfloat16).astype(jnp.float32)

    rotated[...] = jnp.zeros_like(rotated)
    own_score[...] = jnp.zeros_like(own_score)
    own_value[...] = jnp.zeros_like(own_value)
    for kv in range(KVH):
        own_key = turn(head(HQ + kv))
        new_value = head(HQ + KVH + kv)
        for g in range(group):
            query = turn(head(kv * group + g))
            rotated[:, kv * PAD + g, :] = query
            score = jnp.sum(query * own_key, axis=1, keepdims=True) * inv_root
            own_score[:, kv * PAD + g, :] = jnp.broadcast_to(score, (seqs, HD))
            own_value[:, kv * PAD + g, :] = new_value

    @pl.loop(0, seqs)
    def _(s):
        place = lax.broadcasted_iota(jnp.int32, (1, positions), 1) + tp * positions
        is_live = place < lengths[s]
        for kv in range(KVH):
            at = slice(kv * HD, (kv + 1) * HD)
            lanes = slice(kv * PAD, (kv + 1) * PAD)
            query = rotated[s, lanes, :].astype(jnp.bfloat16)
            scores = lax.dot_general(
                query, k_held[s, :, at], (((1,), (1,)), ((), ())),
                preferred_element_type=jnp.float32,
            ) * inv_root
            scores = jnp.where(is_live, scores, jnp.float32(-1e30))
            top = jnp.max(scores, axis=1, keepdims=True)
            weights = jnp.where(is_live, jnp.exp(scores - top), 0.0).astype(jnp.bfloat16)
            total = jnp.sum(weights.astype(jnp.float32), axis=1, keepdims=True)
            parts[tp, 0, s, lanes, :] = jnp.dot(
                weights, v_held[s, :, at], preferred_element_type=jnp.float32
            )
            parts[tp, 1, s, lanes, :] = jnp.broadcast_to(top, (PAD, HD))
            parts[tp, 2, s, lanes, :] = jnp.broadcast_to(total, (PAD, HD))

    send_all(parts, small_sem.at[2], small_sem.at[3])

    for d in range(2, planes - 1):
        relay(d)
    settle(planes - 2)

    @pl.when((core == 1) & (plane == planes - 2))
    def _():
        send_tails(0, up)

    @pl.when((core == 1) & (plane == 1))
    def _():
        send_tails(planes - 1, down)


    landed(parts.at[pl.ds(0, tps - 1)], small_sem.at[3])

    @pl.loop(0, seqs)
    def _(s):
        mine = own_score[s]
        top = mine
        for t in range(tps):
            top = jnp.maximum(top, parts[t, 1, s])
        mine = jnp.exp(mine - top).astype(jnp.bfloat16).astype(jnp.float32)
        numerator, denominator = mine * own_value[s], mine
        for t in range(tps):
            scale = jnp.exp(parts[t, 1, s] - top)
            numerator = numerator + parts[t, 0, s] * scale
            denominator = denominator + parts[t, 2, s] * scale
        rotated[s] = numerator / denominator

    for j in range(HQ):
        row = (j // group) * PAD + j % group
        attended[:, j * HD : (j + 1) * HD] = rotated[:, row, :].astype(attended.dtype)

    @pl.loop(0, w_out.shape[1] // tile)
    def _(i):
        at = pl.ds(pl.multiple_of(i * tile, tile), tile)
        decoded[:, at] = jnp.dot(
            attended[...], w_out[:, at], preferred_element_type=jnp.float32
        ).astype(decoded.dtype)

    sent(bytes_of(tps - 1), a_send.at[0])
    sent(joined.at[pl.ds(0, tps - 1)], small_sem.at[0])
    sent(parts.at[pl.ds(0, tps - 1)], small_sem.at[2])
    for d in range(planes - 2):
        settle(d)
    settle_next(0)
    relay(planes - 1)

    @pl.when((core == 1) & (plane == planes - 1))
    def _():
        take_tails(0)

    @pl.when((core == 1) & (plane == 0))
    def _():
        take_tails(planes - 1)

    settle(planes - 1)
    at_end = (plane == 0) | (plane == planes - 1)

    @pl.when(at_end & (core == 1))
    def _():
        sent(out_rows(2 * tail), t_send.at[1])

    @pl.when(at_end & (core == 0))
    def _():
        landed(out_rows(2 * tail), t_recv.at[len(tails)])

    for d in range(1, planes - 1):
        settle_next(d)

    @pl.when((core == 1) & ((plane == 1) | (plane == planes - 2)))
    def _():
        sent(out_rows(2 * tail), t_send.at[0])


def flush_kernel(decoded, qkv, out, decoded_to, qkv_to, out_to, sems):
    pairs = ((decoded, decoded_to), (qkv, qkv_to), (out, out_to))
    for i, (source, target) in enumerate(pairs):
        cuts = max(c for c in range(1, CUTS + 1) if c == 1 or source.shape[0] % (16 * c) == 0)
        rows = source.shape[0] // cuts
        for j in range(cuts):
            at = pl.ds(j * rows, rows)
            pltpu.make_async_copy(source.at[at], target.at[at], sems.at[i]).start()
    for i, (source, target) in enumerate(pairs):
        pltpu.make_async_copy(source, target, sems.at[i]).wait()


def flush(*arrays):
    return pl.pallas_call(
        flush_kernel,
        out_shape=[jax.ShapeDtypeStruct(x.shape, x.dtype) for x in arrays],
        in_specs=[pl.BlockSpec(memory_space=pltpu.VMEM)] * 3,
        out_specs=[pl.BlockSpec(memory_space=pltpu.HBM)] * 3,
        scratch_shapes=[pltpu.SemaphoreType.DMA((3,))],
        compiler_params=pltpu.CompilerParams(vmem_limit_bytes=2**20),
    )(*arrays)


def fused(mesh, hidden, lengths, old_qkv, old_out, keys, values, new_qkv, new_out):
    reps, tps = mesh.shape["rep"], mesh.shape["tp"]
    planes = reps // 2
    seqs = keys.shape[0]
    rows = new_qkv.shape[0]
    widths = (new_qkv.shape[1] // tps, new_out.shape[1] // tps)
    half = HD // 2
    frequency = ROPE_BASE ** (-2.0 * np.arange(half) / (2 * half))
    frequency = jnp.asarray(np.concatenate([frequency, frequency])[None], jnp.float32)

    sem = pltpu.SemaphoreType.DMA
    whole, anywhere = pl.BlockSpec(memory_space=pltpu.VMEM), pl.BlockSpec(memory_space=pl.ANY)
    in_hbm = pl.BlockSpec(memory_space=pltpu.HBM)
    f32, bf16 = jnp.float32, jnp.bfloat16
    padded = KVH * PAD
    landed = 2 * rows * reps * tps * sum(widths)
    scratch = [sem((1,)), sem((tps - 1, 2)), sem((planes + 1,)), sem((planes, tps // 2)), sem((2,))]
    scratch += [sem((planes,)), sem((planes,)), sem((2,)), sem((5,))]
    scratch += [sem((4,)), sem((7,)), sem((4,)), pltpu.SemaphoreType.REGULAR((3,))]
    scratch += [pltpu.VMEM((rows, new_qkv.shape[1] + new_out.shape[1]), bf16)]
    scratch += [pltpu.VMEM(x.shape, x.dtype) for x in (old_qkv, old_out, keys, values)]
    scratch += [
        pltpu.VMEM((tps, seqs, widths[0]), bf16),
        pltpu.VMEM((seqs, padded, HD), f32),
        pltpu.VMEM((seqs, padded, HD), f32),
        pltpu.VMEM((seqs, padded, HD), f32),
        pltpu.VMEM((tps, 3, seqs, padded, HD), f32),
        pltpu.VMEM((seqs, HQ * HD), bf16),
        pltpu.VMEM((seqs, HD), f32),
        pltpu.VMEM((seqs, HD), f32),
        pltpu.VMEM(hidden.shape, hidden.dtype),
        pltpu.VMEM(frequency.shape, frequency.dtype),
        pltpu.SMEM(lengths.shape, lengths.dtype),
    ]
    return pl.pallas_call(
        functools.partial(step_kernel, planes, tps),
        out_shape=[pltpu.VMEM((seqs, widths[1]), bf16)]
        + [pltpu.VMEM((rows * reps * tps, width), bf16) for width in widths],
        in_specs=[in_hbm] * 9,
        out_specs=[whole] + [anywhere] * 2,
        scratch_shapes=scratch,
        compiler_params=pltpu.CompilerParams(
            collective_id=0, has_side_effects=True, vmem_limit_bytes=VMEM_BYTES - landed - SLACK
        ),
    )(hidden, lengths, frequency, old_qkv, old_out, keys, values, new_qkv, new_out)


def solution(mesh):
    in_specs = (
        P("rep", None),
        P("rep"),
        P(None, "tp"),
        P(None, "tp"),
        P("rep", "tp", None),
        P("rep", "tp", None),
        P(("rep", "tp"), None),
        P(("rep", "tp"), None),
    )
    out_specs = (P("rep", "tp"), P(None, "tp"), P(None, "tp"))

    def step(*args):
        reps, tps = mesh.shape["rep"], mesh.shape["tp"]
        widths = [x.shape[1] // tps for x in args[6:]]
        rows = args[6].shape[0]
        tiled = rows % 16 == 0 and all(width % 128 == 0 for width in widths)
        tiled = tiled and rows > TAIL * 8 and rows * tps * sum(widths) % widths[1] == 0
        if reps % 4 or reps < 6 or tps != 4 or not tiled:
            return (per_device(*args[:6]), *native_move(*args[6:]))
        return tuple(flush(*fused(mesh, *args)))

    return jax.shard_map(
        step, mesh=mesh, in_specs=in_specs, out_specs=out_specs, check_vma=False
    )
```

```python
import functools

import jax
import jax.numpy as jnp
import numpy as np
from jax import lax
from jax.experimental import pallas as pl
from jax.experimental.pallas import tpu as pltpu
from jax.sharding import PartitionSpec as P

HQ = 28
KVH = 4
HD = 128
PAD = 8
CUTS = 28
TAIL = 4
DETOUR = 16
VMEM_BYTES = 67043328
SLACK = 600000
MESH = pl.DeviceIdType.MESH


ROPE_BASE = 1000000.0


def rotate(vectors, positions):
    half_dim = vectors.shape[-1] // 2
    frequency = ROPE_BASE ** (-2.0 * jnp.arange(half_dim, dtype=jnp.float32) / (2 * half_dim))
    angles = positions.astype(jnp.float32)[:, None, None] * frequency
    first_half = vectors[..., :half_dim]
    second_half = vectors[..., half_dim:]
    return jnp.concatenate(
        [
            first_half * jnp.cos(angles) - second_half * jnp.sin(angles),
            second_half * jnp.cos(angles) + first_half * jnp.sin(angles),
        ],
        axis=-1,
    )


def per_device(hidden_state, lengths, old_qkv, old_out, cache_keys, cache_values):
    seq_count = hidden_state.shape[0]
    local_joined = jnp.dot(hidden_state, old_qkv, preferred_element_type=jnp.float32).astype(
        jnp.bfloat16
    )
    joined_rows = lax.all_gather(local_joined, "tp", axis=1, tiled=True)
    q_width = HQ * HD
    k_width = KVH * HD
    group_size = HQ // KVH
    queries = rotate(
        joined_rows[:, :q_width].astype(jnp.float32).reshape(seq_count, HQ, HD), lengths
    ).astype(jnp.bfloat16)
    own_keys = rotate(
        joined_rows[:, q_width : q_width + k_width].astype(jnp.float32).reshape(seq_count, KVH, HD),
        lengths,
    ).astype(jnp.bfloat16)
    own_values = joined_rows[:, q_width + k_width :].reshape(seq_count, KVH, HD)
    inv_root = 1.0 / jnp.sqrt(jnp.float32(HD))
    cache_rows = cache_keys.shape[1]
    grouped = queries.reshape(seq_count, KVH, group_size, HD)
    key_blocks = cache_keys.reshape(seq_count, cache_rows, KVH, HD)
    value_blocks = cache_values.reshape(seq_count, cache_rows, KVH, HD)
    scores = (
        jnp.einsum("skgd,stkd->skgt", grouped, key_blocks, preferred_element_type=jnp.float32)
        * inv_root
    )
    positions = lax.axis_index("tp") * cache_rows + jnp.arange(cache_rows, dtype=jnp.int32)
    live_mask = (positions[None, :] < lengths[:, None])[:, None, None, :]
    scores = jnp.where(live_mask, scores, jnp.float32(-1e30))
    own_score = (
        jnp.sum(grouped.astype(jnp.float32) * own_keys.astype(jnp.float32)[:, :, None, :], axis=-1)
        * inv_root
    )
    local_top = jnp.maximum(jnp.max(scores, axis=-1), own_score)
    top_score = lax.pmax(local_top, "tp")
    weights = jnp.where(live_mask, jnp.exp(scores - top_score[..., None]), jnp.float32(0.0)).astype(
        jnp.bfloat16
    )
    numer_part = jnp.einsum(
        "skgt,stkd->skgd", weights, value_blocks, preferred_element_type=jnp.float32
    )
    denom_part = jnp.sum(weights.astype(jnp.float32), axis=-1)
    numerator, denominator = lax.psum((numer_part, denom_part), "tp")
    own_weight = lax.optimization_barrier(
        jnp.exp(own_score - top_score).astype(jnp.bfloat16)
    ).astype(jnp.float32)
    numerator = numerator + own_weight[..., None] * own_values.astype(jnp.float32)[:, :, None, :]
    denominator = denominator + own_weight
    attended = (numerator / denominator[..., None]).reshape(seq_count, q_width).astype(jnp.bfloat16)
    decoded = jnp.dot(attended, old_out, preferred_element_type=jnp.float32).astype(jnp.bfloat16)
    return decoded


def native_move(new_qkv, new_out):
    def move(block):
        piece = lax.all_to_all(block, "tp", split_axis=1, concat_axis=0, tiled=True)
        return lax.all_gather(piece, "rep", axis=0, tiled=True)

    return move(new_qkv), move(new_out)


def flip(index, bits, size):
    out = index
    bit = 1
    while bit < size:
        if (bits // bit) % 2:
            out = out + bit - 2 * bit * ((index // bit) % 2)
        bit *= 2
    return out


def step_kernel(
    planes, tps,
    hidden_in, lengths_in, frequency_in, old_qkv, old_out, keys, values, new_qkv, new_out,
    decoded, qkv_full, out_full,
    a_send, a_recv, z_send, z_recv, z_last, s_send, s_recv, t_send, t_recv, own_sem,
    load_sem, small_sem, met, d_send, d_recv,
    stage, detour,
    w_qkv, w_out, k_held, v_held, joined, rotated, own_score, own_value, parts, attended,
    cosine, sine, hidden, frequency, lengths,
):
    rep, tp = lax.axis_index("rep"), lax.axis_index("tp")
    plane, core = rep // 2, rep % 2
    rows = new_qkv.shape[0]
    fulls = (qkv_full, out_full)
    widths = (qkv_full.shape[1], out_full.shape[1])
    bases = (0, new_qkv.shape[1])
    up = (jnp.minimum(plane + 1, planes - 1) * 2 + core, tp)
    down = (jnp.maximum(plane - 1, 0) * 2 + core, tp)
    twin = (plane * 2 + 1 - core, tp)
    peers = [(rep, flip(tp, k, tps)) for k in range(1, tps)]
    near = [k for k in range(1, tps) if k & (k - 1) == 0]
    far = [k for k in range(1, tps) if k & (k - 1)]
    can_up, can_down = plane < planes - 1, plane > 0

    half = tps // 2

    def at_rows(source_plane, source_core, first, count, w):
        start = ((source_plane * 2 + source_core) * tps) * rows + first
        return fulls[w].at[pl.ds(pl.multiple_of(start, 16), count)]

    def piece_rows(source_plane, source_core, k, w):
        return at_rows(source_plane, source_core, flip(tp, k, tps) * rows, rows, w)

    mine = [
        pltpu.make_async_copy(
            source.at[:, pl.ds(pl.multiple_of(tp * widths[w], 128), widths[w])],
            piece_rows(plane, core, 0, w), own_sem.at[w],
        )
        for w, source in enumerate((new_qkv, new_out))
    ]
    staged = [
        pltpu.make_async_copy(
            source, stage.at[:, pl.ds(bases[w], source.shape[1])], own_sem.at[2 + w]
        )
        for w, source in enumerate((new_qkv, new_out))
    ]
    for copy in mine + staged:
        copy.start()
    barrier = pltpu.get_barrier_semaphore()
    beside = [twin] + [peers[k - 1] for k in near]

    def tell(semaphore, device):
        pl.semaphore_signal(semaphore, inc=1, device_id=device, device_id_type=MESH)

    @pl.when(can_up)
    def _():
        tell(barrier, up)

    @pl.when(can_down & (plane != 2))
    def _():
        tell(barrier, down)

    @pl.when(plane != 1)
    def _():
        for device in beside:
            tell(barrier, device)

    small = [
        pltpu.make_async_copy(source, target, load_sem.at[4 + i])
        for i, (source, target) in enumerate(
            ((hidden_in, hidden), (frequency_in, frequency), (lengths_in, lengths))
        )
    ]

    @pl.when(plane == 1)
    def _():
        pl.semaphore_wait(barrier, 1)

    @pl.when((plane != 1) & can_up & can_down)
    def _():
        pl.semaphore_wait(barrier, len(beside) + 2)

    @pl.when(jnp.logical_not(can_up & can_down))
    def _():
        pl.semaphore_wait(barrier, len(beside) + 1)

    def remote(source, target, send, recv, device):
        return pltpu.make_async_remote_copy(
            src_ref=source, dst_ref=target, send_sem=send, recv_sem=recv,
            device_id=device, device_id_type=MESH,
        )

    def sent(ref, sem):
        remote(ref, ref, sem, sem, twin).wait_send()

    def landed(ref, sem):
        remote(ref, ref, sem, sem, twin).wait_recv()

    def pair_first(h):
        return (flip(tp, 2 * h, tps) // 2) * 2 * rows

    tail = TAIL * 16
    tails = [(1, first, count) for first, count in ((2 * rows - tail, tail - 16), (2 * rows - 16, 16))]
    tails = [(c, part) for part in tails for c in (1, 0)]

    def parts_of(h, last):
        if last and h == half - 1:
            return [(0, 0, 2 * rows, 0), (1, 0, 2 * rows - tail, 1)]
        return [(w, 0, 2 * rows, None) for w in range(2)]

    def part_rows(source_plane, source_core, h, part):
        w, first, count = part[:3]
        return at_rows(source_plane, source_core, pair_first(h) + first, count, w)

    def part_sem(source_plane, h, part):
        return z_recv.at[source_plane, h] if part[3] is None else z_last.at[part[3]]

    def bytes_of(parts):
        return stage.at[:, pl.ds(0, stage.shape[1] // tps * parts)]

    def out_rows(count):
        return out_full.at[pl.ds(0, count)]

    def block_bytes(last):
        if last:
            return out_rows(rows * tps * sum(widths) // widths[1] - tail)
        return stage

    def send_tails(source_plane, device):
        for i, (c, part) in enumerate(tails):
            ref = part_rows(source_plane, c, half - 1, part)
            remote(ref, ref, t_send.at[0], t_recv.at[i], device).start()

    def take_tails(source_plane):
        for i, (c, part) in enumerate(tails):
            ref = part_rows(source_plane, c, half - 1, part)
            landed(ref, t_recv.at[i])
            remote(ref, ref, t_send.at[1], t_recv.at[len(tails)], twin).start()

    def column(w, t):
        start = bases[w] + t * widths[w]
        return stage.at[:, pl.ds(pl.multiple_of(start, 128), widths[w])]

    def in_plane(k, w):
        remote(
            column(w, flip(tp, k, tps)), piece_rows(plane, core, 0, w),
            a_send.at[0], a_recv.at[k - 1, w], peers[k - 1],
        ).start()

    def own_up(k, w):
        ref = piece_rows(plane, core, k, w)

        @pl.when(can_up)
        def _():
            remote(ref, ref, z_send.at[plane], z_recv.at[plane, k // 2], up).start()

    def own_down(k, w):
        ref = piece_rows(plane, core, k, w)

        def send(ref):
            remote(ref, ref, z_send.at[plane + 1], z_recv.at[plane, k // 2], down).start()

        if w and k:
            short = detoured & (core == (k + 1) % 2)

            @pl.when(short)
            def _():
                send(at_rows(plane, core, flip(tp, k, tps) * rows, rows - DETOUR, w))

            @pl.when(can_down & jnp.logical_not(short))
            def _():
                send(ref)

        else:

            @pl.when(can_down)
            def _():
                send(ref)

    def own_twin(k, w):
        ref = piece_rows(plane, core, k, w)
        remote(ref, ref, s_send.at[plane], s_recv.at[plane], twin).start()

    detoured = (plane == 1) & (tp == 0)
    carries = (tp != 0) & (core == (tp + 1) % 2)

    def detour_down():
        @pl.when((plane == 1) & carries)
        def _():
            source = stage.at[pl.ds(rows - DETOUR, DETOUR), pl.ds(bases[1], widths[1])]
            remote(source, detour, d_send.at[0], d_recv.at[0], down).start()

    def detour_across():
        @pl.when((plane == 0) & carries)
        def _():
            landed(detour, d_recv.at[0])
            target = at_rows(1, core, tp * rows + rows - DETOUR, DETOUR, 1)
            remote(detour, target, d_send.at[0], z_recv.at[1, tp // 2], (rep, jnp.int32(0))).start()

    def take(source_plane, h, last, parts, forward, slot, onward):
        if last:
            (part,) = parts
            landed(part_rows(source_plane, core, h, part), part_sem(source_plane, h, part))
        else:
            landed(bytes_of(2), z_recv.at[source_plane, h])
        if forward is not None:
            can, device = forward

            @pl.when(can)
            def _():
                for part in onward:
                    ref = part_rows(source_plane, core, h, part)
                    remote(
                        ref, ref, z_send.at[slot], part_sem(source_plane, h, part), device
                    ).start()

        for part in parts:
            ref = part_rows(source_plane, core, h, part)
            remote(ref, ref, s_send.at[source_plane], s_recv.at[source_plane], twin).start()

    def relay(d):
        ends = d == planes - 1
        for h in range(half):
            cuts = parts_of(h, ends)
            onward = parts_of(h, d == planes - 2)
            single = ends and h == half - 1
            for parts in [[part] for part in cuts] if single else [cuts]:

                @pl.when(plane >= d)
                def _():
                    take(plane - d, h, single, parts, None if ends else (can_up, up), plane - d, onward)

                @pl.when(plane + d < planes)
                def _():
                    take(
                        plane + d, h, single, parts,
                        None if ends else (can_down, down), plane + d + 1, onward,
                    )

    def settle_twin(source_plane, last):
        landed(block_bytes(last), s_recv.at[source_plane])
        sent(block_bytes(last), s_send.at[source_plane])

    def settle_own():
        cut = rows * tps * sum(widths) // widths[1]
        shorts = [
            (c, cut - DETOUR * sum((k + 1) % 2 == c for k in range(1, tps))) for c in range(2)
        ]

        @pl.when(can_up)
        def _():
            sent(stage, z_send.at[plane])

        @pl.when(can_down & jnp.logical_not(detoured))
        def _():
            sent(stage, z_send.at[plane + 1])

        for c, count in shorts:

            @pl.when(detoured & (core == c))
            def _():
                sent(out_rows(count), z_send.at[plane + 1])

        @pl.when((plane < 2) & carries)
        def _():
            sent(detour, d_send.at[0])

    def settle_next(d):
        @pl.when((plane >= d) & can_up)
        def _():
            sent(block_bytes(d == planes - 2), z_send.at[plane - d])

        @pl.when((plane + d < planes) & can_down)
        def _():
            sent(block_bytes(d == planes - 2), z_send.at[plane + d + 1])

    def settle(d):
        @pl.when(plane >= d)
        def _():
            settle_twin(plane - d, d == planes - 1)

        if d:

            @pl.when(plane + d < planes)
            def _():
                settle_twin(plane + d, d == planes - 1)

    for w in range(2):
        mine[w].wait()
        own_down(0, w)

    def open_plane():
        for w in (1, 0):
            staged[w].wait()
            for k in near:
                in_plane(k, w)
        for w in range(2):
            own_twin(0, w)

    @pl.when(plane == 0)
    def _():
        for device in beside:
            tell(met.at[0], device)

    @pl.when(plane == 2)
    def _():
        tell(met.at[1], down)

    @pl.when(plane != 1)
    def _():
        for w in range(2):
            own_up(0, w)
        open_plane()

    @pl.when(plane == 0)
    def _():
        pl.semaphore_wait(met.at[0], len(beside))
        tell(met.at[2], up)

    @pl.when(plane == 1)
    def _():
        pl.semaphore_wait(met.at[2], 1)
        open_plane()
        detour_down()
        pl.semaphore_wait(met.at[1], 1)
        for w in range(2):
            own_up(0, w)

    loads = [
        pltpu.make_async_copy(source, target, load_sem.at[i])
        for i, (source, target) in enumerate(
            ((old_qkv, w_qkv), (keys, k_held), (values, v_held), (old_out, w_out))
        )
    ]
    for copy in loads + small:
        copy.start()
    arrivals = [(k, w) for w in (1, 0) for k in near] + [(k, w) for k in far for w in (1, 0)]
    for k, w in arrivals:
        landed(piece_rows(plane, core, k, w), a_recv.at[k - 1, w])
        own_down(k, w)
        own_up(k, w)
        own_twin(k, w)
        if (k, w) == arrivals[0]:
            for j in far:
                for v in (1, 0):
                    in_plane(j, v)

    detour_across()
    for copy in small:
        copy.wait()
    seqs = hidden.shape[0]
    lane = lax.broadcasted_iota(jnp.int32, (1, HD), 1)
    for s in range(seqs):
        angles = lengths[s].astype(jnp.float32) * frequency[...]
        cosine[s : s + 1, :] = jnp.cos(angles)
        sine[s : s + 1, :] = jnp.where(lane < HD // 2, -jnp.sin(angles), jnp.sin(angles))
    tile = 128
    loads[0].wait()

    @pl.loop(0, w_qkv.shape[1] // tile)
    def _(i):
        at = pl.ds(pl.multiple_of(i * tile, tile), tile)
        joined[tp, :, at] = jnp.dot(
            hidden[...], w_qkv[:, at], preferred_element_type=jnp.float32
        ).astype(joined.dtype)

    def send_all(ref, send, recv):
        for k in range(1, tps):
            remote(ref.at[tp], ref.at[tp], send, recv, peers[k - 1]).start()

    send_all(joined, small_sem.at[0], small_sem.at[1])

    relay(1)

    landed(joined.at[pl.ds(0, tps - 1)], small_sem.at[1])
    for copy in loads[1:]:
        copy.wait()

    group = HQ // KVH
    positions = k_held.shape[1]
    per_slot = joined.shape[2] // HD
    inv_root = 1.0 / jnp.sqrt(jnp.float32(HD))

    def head(j):
        at = (j % per_slot) * HD
        return joined[j // per_slot, :, at : at + HD].astype(jnp.float32)

    def turn(v):
        swapped = jnp.concatenate([v[:, HD // 2 :], v[:, : HD // 2]], axis=1)
        return (v * cosine[...] + swapped * sine[...]).astype(jnp.bfloat16).astype(jnp.float32)

    rotated[...] = jnp.zeros_like(rotated)
    own_score[...] = jnp.zeros_like(own_score)
    own_value[...] = jnp.zeros_like(own_value)
    for kv in range(KVH):
        own_key = turn(head(HQ + kv))
        new_value = head(HQ + KVH + kv)
        for g in range(group):
            query = turn(head(kv * group + g))
            rotated[:, kv * PAD + g, :] = query
            score = jnp.sum(query * own_key, axis=1, keepdims=True) * inv_root
            own_score[:, kv * PAD + g, :] = jnp.broadcast_to(score, (seqs, HD))
            own_value[:, kv * PAD + g, :] = new_value

    @pl.loop(0, seqs)
    def _(s):
        place = lax.broadcasted_iota(jnp.int32, (1, positions), 1) + tp * positions
        is_live = place < lengths[s]
        for kv in range(KVH):
            at = slice(kv * HD, (kv + 1) * HD)
            lanes = slice(kv * PAD, (kv + 1) * PAD)
            query = rotated[s, lanes, :].astype(jnp.bfloat16)
            scores = lax.dot_general(
                query, k_held[s, :, at], (((1,), (1,)), ((), ())),
                preferred_element_type=jnp.float32,
            ) * inv_root
            scores = jnp.where(is_live, scores, jnp.float32(-1e30))
            top = jnp.max(scores, axis=1, keepdims=True)
            weights = jnp.where(is_live, jnp.exp(scores - top), 0.0).astype(jnp.bfloat16)
            total = jnp.sum(weights.astype(jnp.float32), axis=1, keepdims=True)
            parts[tp, 0, s, lanes, :] = jnp.dot(
                weights, v_held[s, :, at], preferred_element_type=jnp.float32
            )
            parts[tp, 1, s, lanes, :] = jnp.broadcast_to(top, (PAD, HD))
            parts[tp, 2, s, lanes, :] = jnp.broadcast_to(total, (PAD, HD))

    send_all(parts, small_sem.at[2], small_sem.at[3])

    for d in range(2, planes - 1):
        relay(d)
    settle(planes - 2)

    @pl.when((core == 1) & (plane == planes - 2))
    def _():
        send_tails(0, up)

    @pl.when((core == 1) & (plane == 1))
    def _():
        send_tails(planes - 1, down)


    landed(parts.at[pl.ds(0, tps - 1)], small_sem.at[3])

    @pl.loop(0, seqs)
    def _(s):
        mine = own_score[s]
        top = mine
        for t in range(tps):
            top = jnp.maximum(top, parts[t, 1, s])
        mine = jnp.exp(mine - top).astype(jnp.bfloat16).astype(jnp.float32)
        numerator, denominator = mine * own_value[s], mine
        for t in range(tps):
            scale = jnp.exp(parts[t, 1, s] - top)
            numerator = numerator + parts[t, 0, s] * scale
            denominator = denominator + parts[t, 2, s] * scale
        rotated[s] = numerator / denominator

    for j in range(HQ):
        row = (j // group) * PAD + j % group
        attended[:, j * HD : (j + 1) * HD] = rotated[:, row, :].astype(attended.dtype)

    @pl.loop(0, w_out.shape[1] // tile)
    def _(i):
        at = pl.ds(pl.multiple_of(i * tile, tile), tile)
        decoded[:, at] = jnp.dot(
            attended[...], w_out[:, at], preferred_element_type=jnp.float32
        ).astype(decoded.dtype)

    sent(bytes_of(tps - 1), a_send.at[0])
    sent(joined.at[pl.ds(0, tps - 1)], small_sem.at[0])
    sent(parts.at[pl.ds(0, tps - 1)], small_sem.at[2])
    for d in range(planes - 2):
        settle(d)
    settle_own()
    relay(planes - 1)

    @pl.when((core == 1) & (plane == planes - 1))
    def _():
        take_tails(0)

    @pl.when((core == 1) & (plane == 0))
    def _():
        take_tails(planes - 1)

    settle(planes - 1)
    at_end = (plane == 0) | (plane == planes - 1)

    @pl.when(at_end & (core == 1))
    def _():
        sent(out_rows(2 * tail), t_send.at[1])

    @pl.when(at_end & (core == 0))
    def _():
        landed(out_rows(2 * tail), t_recv.at[len(tails)])

    for d in range(1, planes - 1):
        settle_next(d)

    @pl.when((core == 1) & ((plane == 1) | (plane == planes - 2)))
    def _():
        sent(out_rows(2 * tail), t_send.at[0])


def flush_kernel(decoded, qkv, out, decoded_to, qkv_to, out_to, sems):
    pairs = ((decoded, decoded_to), (qkv, qkv_to), (out, out_to))
    for i, (source, target) in enumerate(pairs):
        cuts = max(c for c in range(1, CUTS + 1) if c == 1 or source.shape[0] % (16 * c) == 0)
        rows = source.shape[0] // cuts
        for j in range(cuts):
            at = pl.ds(j * rows, rows)
            pltpu.make_async_copy(source.at[at], target.at[at], sems.at[i]).start()
    for i, (source, target) in enumerate(pairs):
        pltpu.make_async_copy(source, target, sems.at[i]).wait()


def flush(*arrays):
    return pl.pallas_call(
        flush_kernel,
        out_shape=[jax.ShapeDtypeStruct(x.shape, x.dtype) for x in arrays],
        in_specs=[pl.BlockSpec(memory_space=pltpu.VMEM)] * 3,
        out_specs=[pl.BlockSpec(memory_space=pltpu.HBM)] * 3,
        scratch_shapes=[pltpu.SemaphoreType.DMA((3,))],
        compiler_params=pltpu.CompilerParams(vmem_limit_bytes=2**20),
    )(*arrays)


def fused(mesh, hidden, lengths, old_qkv, old_out, keys, values, new_qkv, new_out):
    reps, tps = mesh.shape["rep"], mesh.shape["tp"]
    planes = reps // 2
    seqs = keys.shape[0]
    rows = new_qkv.shape[0]
    widths = (new_qkv.shape[1] // tps, new_out.shape[1] // tps)
    half = HD // 2
    frequency = ROPE_BASE ** (-2.0 * np.arange(half) / (2 * half))
    frequency = jnp.asarray(np.concatenate([frequency, frequency])[None], jnp.float32)

    sem = pltpu.SemaphoreType.DMA
    whole, anywhere = pl.BlockSpec(memory_space=pltpu.VMEM), pl.BlockSpec(memory_space=pl.ANY)
    in_hbm = pl.BlockSpec(memory_space=pltpu.HBM)
    f32, bf16 = jnp.float32, jnp.bfloat16
    padded = KVH * PAD
    landed = 2 * rows * reps * tps * sum(widths)
    scratch = [sem((1,)), sem((tps - 1, 2)), sem((planes + 1,)), sem((planes, tps // 2)), sem((2,))]
    scratch += [sem((planes,)), sem((planes,)), sem((2,)), sem((5,))]
    scratch += [sem((4,)), sem((7,)), sem((4,)), pltpu.SemaphoreType.REGULAR((3,))]
    scratch += [sem((1,)), sem((1,))]
    scratch += [pltpu.VMEM((rows, new_qkv.shape[1] + new_out.shape[1]), bf16)]
    scratch += [pltpu.VMEM((DETOUR, widths[1]), bf16)]
    scratch += [pltpu.VMEM(x.shape, x.dtype) for x in (old_qkv, old_out, keys, values)]
    scratch += [
        pltpu.VMEM((tps, seqs, widths[0]), bf16),
        pltpu.VMEM((seqs, padded, HD), f32),
        pltpu.VMEM((seqs, padded, HD), f32),
        pltpu.VMEM((seqs, padded, HD), f32),
        pltpu.VMEM((tps, 3, seqs, padded, HD), f32),
        pltpu.VMEM((seqs, HQ * HD), bf16),
        pltpu.VMEM((seqs, HD), f32),
        pltpu.VMEM((seqs, HD), f32),
        pltpu.VMEM(hidden.shape, hidden.dtype),
        pltpu.VMEM(frequency.shape, frequency.dtype),
        pltpu.SMEM(lengths.shape, lengths.dtype),
    ]
    return pl.pallas_call(
        functools.partial(step_kernel, planes, tps),
        out_shape=[pltpu.VMEM((seqs, widths[1]), bf16)]
        + [pltpu.VMEM((rows * reps * tps, width), bf16) for width in widths],
        in_specs=[in_hbm] * 9,
        out_specs=[whole] + [anywhere] * 2,
        scratch_shapes=scratch,
        compiler_params=pltpu.CompilerParams(
            collective_id=0, has_side_effects=True, vmem_limit_bytes=VMEM_BYTES - landed - SLACK
        ),
    )(hidden, lengths, frequency, old_qkv, old_out, keys, values, new_qkv, new_out)


def solution(mesh):
    in_specs = (
        P("rep", None),
        P("rep"),
        P(None, "tp"),
        P(None, "tp"),
        P("rep", "tp", None),
        P("rep", "tp", None),
        P(("rep", "tp"), None),
        P(("rep", "tp"), None),
    )
    out_specs = (P("rep", "tp"), P(None, "tp"), P(None, "tp"))

    def step(*args):
        reps, tps = mesh.shape["rep"], mesh.shape["tp"]
        widths = [x.shape[1] // tps for x in args[6:]]
        rows = args[6].shape[0]
        tiled = rows % 16 == 0 and all(width % 128 == 0 for width in widths)
        tiled = tiled and rows > max(TAIL * 8, DETOUR) and rows * tps * sum(widths) % widths[1] == 0
        if reps % 4 or reps < 6 or tps != 4 or not tiled:
            return (per_device(*args[:6]), *native_move(*args[6:]))
        return tuple(flush(*fused(mesh, *args)))

    return jax.shard_map(
        step, mesh=mesh, in_specs=in_specs, out_specs=out_specs, check_vma=False
    )
```

```python
import functools

import jax
import jax.numpy as jnp
import numpy as np
from jax import lax
from jax.experimental import pallas as pl
from jax.experimental.pallas import tpu as pltpu
from jax.sharding import PartitionSpec as P

HQ = 28
KVH = 4
HD = 128
PAD = 8
CUTS = 56
TAIL = 4
DETOUR = 16
VMEM_BYTES = 67043328
SLACK = 600000
MESH = pl.DeviceIdType.MESH


ROPE_BASE = 1000000.0


def rotate(vectors, positions):
    half_dim = vectors.shape[-1] // 2
    frequency = ROPE_BASE ** (-2.0 * jnp.arange(half_dim, dtype=jnp.float32) / (2 * half_dim))
    angles = positions.astype(jnp.float32)[:, None, None] * frequency
    first_half = vectors[..., :half_dim]
    second_half = vectors[..., half_dim:]
    return jnp.concatenate(
        [
            first_half * jnp.cos(angles) - second_half * jnp.sin(angles),
            second_half * jnp.cos(angles) + first_half * jnp.sin(angles),
        ],
        axis=-1,
    )


def per_device(hidden_state, lengths, old_qkv, old_out, cache_keys, cache_values):
    seq_count = hidden_state.shape[0]
    local_joined = jnp.dot(hidden_state, old_qkv, preferred_element_type=jnp.float32).astype(
        jnp.bfloat16
    )
    joined_rows = lax.all_gather(local_joined, "tp", axis=1, tiled=True)
    q_width = HQ * HD
    k_width = KVH * HD
    group_size = HQ // KVH
    queries = rotate(
        joined_rows[:, :q_width].astype(jnp.float32).reshape(seq_count, HQ, HD), lengths
    ).astype(jnp.bfloat16)
    own_keys = rotate(
        joined_rows[:, q_width : q_width + k_width].astype(jnp.float32).reshape(seq_count, KVH, HD),
        lengths,
    ).astype(jnp.bfloat16)
    own_values = joined_rows[:, q_width + k_width :].reshape(seq_count, KVH, HD)
    inv_root = 1.0 / jnp.sqrt(jnp.float32(HD))
    cache_rows = cache_keys.shape[1]
    grouped = queries.reshape(seq_count, KVH, group_size, HD)
    key_blocks = cache_keys.reshape(seq_count, cache_rows, KVH, HD)
    value_blocks = cache_values.reshape(seq_count, cache_rows, KVH, HD)
    scores = (
        jnp.einsum("skgd,stkd->skgt", grouped, key_blocks, preferred_element_type=jnp.float32)
        * inv_root
    )
    positions = lax.axis_index("tp") * cache_rows + jnp.arange(cache_rows, dtype=jnp.int32)
    live_mask = (positions[None, :] < lengths[:, None])[:, None, None, :]
    scores = jnp.where(live_mask, scores, jnp.float32(-1e30))
    own_score = (
        jnp.sum(grouped.astype(jnp.float32) * own_keys.astype(jnp.float32)[:, :, None, :], axis=-1)
        * inv_root
    )
    local_top = jnp.maximum(jnp.max(scores, axis=-1), own_score)
    top_score = lax.pmax(local_top, "tp")
    weights = jnp.where(live_mask, jnp.exp(scores - top_score[..., None]), jnp.float32(0.0)).astype(
        jnp.bfloat16
    )
    numer_part = jnp.einsum(
        "skgt,stkd->skgd", weights, value_blocks, preferred_element_type=jnp.float32
    )
    denom_part = jnp.sum(weights.astype(jnp.float32), axis=-1)
    numerator, denominator = lax.psum((numer_part, denom_part), "tp")
    own_weight = lax.optimization_barrier(
        jnp.exp(own_score - top_score).astype(jnp.bfloat16)
    ).astype(jnp.float32)
    numerator = numerator + own_weight[..., None] * own_values.astype(jnp.float32)[:, :, None, :]
    denominator = denominator + own_weight
    attended = (numerator / denominator[..., None]).reshape(seq_count, q_width).astype(jnp.bfloat16)
    decoded = jnp.dot(attended, old_out, preferred_element_type=jnp.float32).astype(jnp.bfloat16)
    return decoded


def native_move(new_qkv, new_out):
    def move(block):
        piece = lax.all_to_all(block, "tp", split_axis=1, concat_axis=0, tiled=True)
        return lax.all_gather(piece, "rep", axis=0, tiled=True)

    return move(new_qkv), move(new_out)


def flip(index, bits, size):
    out = index
    bit = 1
    while bit < size:
        if (bits // bit) % 2:
            out = out + bit - 2 * bit * ((index // bit) % 2)
        bit *= 2
    return out


def step_kernel(
    planes, tps,
    hidden_in, lengths_in, frequency_in, old_qkv, old_out, keys, values, new_qkv, new_out,
    decoded, qkv_full, out_full,
    a_recv, z_send, z_recv, s_send, s_recv, t_recv, x_recv, local, met,
    stage, detour,
    weights, caches, joined, rotated, own_score, own_value, parts, attended,
    cosine, sine, hidden, frequency, lengths,
):
    rep, tp = lax.axis_index("rep"), lax.axis_index("tp")
    plane, core = rep // 2, rep % 2
    rows = new_qkv.shape[0]
    fulls = (qkv_full, out_full)
    widths = (qkv_full.shape[1], out_full.shape[1])
    bases = (0, new_qkv.shape[1])
    up = (jnp.minimum(plane + 1, planes - 1) * 2 + core, tp)
    down = (jnp.maximum(plane - 1, 0) * 2 + core, tp)
    twin = (plane * 2 + 1 - core, tp)
    peers = [(rep, flip(tp, k, tps)) for k in range(1, tps)]
    near = [k for k in range(1, tps) if k & (k - 1) == 0]
    far = [k for k in range(1, tps) if k & (k - 1)]
    can_up, can_down = plane < planes - 1, plane > 0

    half = tps // 2

    def at_rows(source_plane, source_core, first, count, w):
        start = ((source_plane * 2 + source_core) * tps) * rows + first
        return fulls[w].at[pl.ds(pl.multiple_of(start, 16), count)]

    def piece_rows(source_plane, source_core, k, w):
        return at_rows(source_plane, source_core, flip(tp, k, tps) * rows, rows, w)

    mine = [
        pltpu.make_async_copy(
            source.at[:, pl.ds(pl.multiple_of(tp * widths[w], 128), widths[w])],
            piece_rows(plane, core, 0, w), local.at[w],
        )
        for w, source in enumerate((new_qkv, new_out))
    ]
    staged = [
        pltpu.make_async_copy(
            source, stage.at[:, pl.ds(bases[w], source.shape[1])], local.at[2]
        )
        for w, source in enumerate((new_qkv, new_out))
    ]
    for copy in mine:
        copy.start()
    barrier = pltpu.get_barrier_semaphore()
    beside = [twin] + [peers[k - 1] for k in near]

    def tell(semaphore, device):
        pl.semaphore_signal(semaphore, inc=1, device_id=device, device_id_type=MESH)

    @pl.when(can_up)
    def _():
        tell(barrier, up)

    @pl.when(can_down & (plane != 2))
    def _():
        tell(barrier, down)

    @pl.when(plane != 1)
    def _():
        for device in beside:
            tell(barrier, device)
        for copy in staged:
            copy.start()

    small = [
        pltpu.make_async_copy(source, target, local.at[i])
        for i, (source, target) in enumerate(
            ((hidden_in, hidden), (frequency_in, frequency), (lengths_in, lengths))
        )
    ]

    @pl.when(plane == 1)
    def _():
        pl.semaphore_wait(barrier, 1)

    @pl.when((plane != 1) & can_up & can_down)
    def _():
        pl.semaphore_wait(barrier, len(beside) + 2)

    @pl.when(jnp.logical_not(can_up & can_down))
    def _():
        pl.semaphore_wait(barrier, len(beside) + 1)

    def remote(source, target, send, recv, device):
        return pltpu.make_async_remote_copy(
            src_ref=source, dst_ref=target, send_sem=send, recv_sem=recv,
            device_id=device, device_id_type=MESH,
        )

    def sent(ref, sem):
        remote(ref, ref, sem, sem, twin).wait_send()

    def landed(ref, sem):
        remote(ref, ref, sem, sem, twin).wait_recv()

    def pair_first(h):
        return (flip(tp, 2 * h, tps) // 2) * 2 * rows

    tail = TAIL * 16
    tails = [(1, first, count) for first, count in ((2 * rows - tail, tail - 16), (2 * rows - 16, 16))]
    tails = [(c, part) for part in tails for c in (1, 0)]

    def parts_of(h, last):
        if last and h == half - 1:
            return [(0, 0, 2 * rows, 0), (1, 0, 2 * rows - tail, 1)]
        return [(w, 0, 2 * rows, 0) for w in range(2)]

    def part_rows(source_plane, source_core, h, part):
        w, first, count = part[:3]
        return at_rows(source_plane, source_core, pair_first(h) + first, count, w)

    def part_sem(index, h, part):
        return x_recv.at[0] if part[3] else z_recv.at[index, h]

    def bytes_of(parts):
        return stage.at[:, pl.ds(0, stage.shape[1] // tps * parts)]

    def out_rows(count):
        return out_full.at[pl.ds(0, count)]

    def send_tails(source_plane, device):
        for i, (c, part) in enumerate(tails):
            ref = part_rows(source_plane, c, half - 1, part)
            remote(ref, ref, local.at[6], t_recv.at[i], device).start()

    def take_tails(source_plane):
        for i, (c, part) in enumerate(tails):
            ref = part_rows(source_plane, c, half - 1, part)
            landed(ref, t_recv.at[i])
            remote(ref, ref, local.at[6], t_recv.at[len(tails)], twin).start()

    def column(w, t):
        start = bases[w] + t * widths[w]
        return stage.at[:, pl.ds(pl.multiple_of(start, 128), widths[w])]

    def in_plane(k, w):
        remote(
            column(w, flip(tp, k, tps)), piece_rows(plane, core, 0, w),
            local.at[5], a_recv.at[k - 1, w], peers[k - 1],
        ).start()

    def own_up(k, w):
        ref = piece_rows(plane, core, k, w)

        @pl.when(can_up)
        def _():
            remote(ref, ref, z_send.at[0], z_recv.at[plane, k // 2], up).start()

    def own_down(k, w):
        ref = piece_rows(plane, core, k, w)

        def send(ref):
            remote(ref, ref, z_send.at[1], z_recv.at[plane - 1, k // 2], down).start()

        if w and k:
            short = detoured & (core == (k + 1) % 2)

            @pl.when(short)
            def _():
                send(at_rows(plane, core, flip(tp, k, tps) * rows, rows - DETOUR, w))

            @pl.when(can_down & jnp.logical_not(short))
            def _():
                send(ref)

        else:

            @pl.when(can_down)
            def _():
                send(ref)

    def own_twin(k, w):
        ref = piece_rows(plane, core, k, w)
        remote(ref, ref, s_send.at[0], s_recv.at[0], twin).start()

    detoured = (plane == 1) & (tp == 0)
    carries = (tp != 0) & (core == (tp + 1) % 2)

    def detour_down():
        @pl.when((plane == 1) & carries)
        def _():
            source = stage.at[pl.ds(rows - DETOUR, DETOUR), pl.ds(bases[1], widths[1])]
            remote(source, detour, local.at[6], x_recv.at[1], down).start()

    def detour_across():
        @pl.when((plane == 0) & carries)
        def _():
            landed(detour, x_recv.at[1])
            target = at_rows(1, core, tp * rows + rows - DETOUR, DETOUR, 1)
            remote(detour, target, local.at[6], z_recv.at[0, tp // 2], (rep, jnp.int32(0))).start()

    def take(source_plane, index, h, single, parts, far, can, device, way, onward):
        if single:
            (part,) = parts
            landed(part_rows(source_plane, core, h, part), part_sem(index, h, part))
        else:
            landed(bytes_of(2), z_recv.at[index, h])
        if onward:

            @pl.when(can)
            def _():
                for part in onward:
                    ref = part_rows(source_plane, core, h, part)
                    sem = part_sem(source_plane - way, h, part)
                    remote(ref, ref, z_send.at[way], sem, device).start()

        for part in parts:
            ref = part_rows(source_plane, core, h, part)
            remote(ref, ref, s_send.at[far], s_recv.at[far], twin).start()

    def farthest(source_plane):
        other = jnp.where(plane < planes // 2, planes - 1, 0)
        return jnp.where(source_plane == other, 1, 0)

    def relay(d):
        ends = d == planes - 1
        for h in range(half):
            cuts = parts_of(h, ends)
            onward = [] if ends else parts_of(h, d == planes - 2)
            single = ends and h == half - 1
            for parts in [[part] for part in cuts] if single else [cuts]:

                @pl.when(plane >= d)
                def _():
                    s = plane - d
                    take(s, s, h, single, parts, farthest(s), can_up, up, 0, onward)

                @pl.when(plane + d < planes)
                def _():
                    s = plane + d
                    take(s, s - 1, h, single, parts, farthest(s), can_down, down, 1, onward)

    block = rows * tps * sum(widths) // widths[1]

    def settle_twin(count, far):
        landed(out_rows(count), s_recv.at[far])
        sent(out_rows(count), s_send.at[far])

    def settle_next(p):
        @pl.when(plane == p)
        def _():
            for way, count in ((0, p + 1), (1, planes - p)):
                if p == (planes - 1, 0)[way]:
                    continue
                total = count * block - (tail if p == (planes - 2, 1)[way] else 0)
                if p != 1 or way == 0:
                    sent(out_rows(total), z_send.at[way])
                    continue

                @pl.when(tp != 0)
                def _():
                    sent(out_rows(total), z_send.at[way])

                for c in range(2):
                    cut = DETOUR * sum((k + 1) % 2 == c for k in range(1, tps))

                    @pl.when((tp == 0) & (core == c))
                    def _():
                        sent(out_rows(total - cut), z_send.at[way])

    for w in range(2):
        mine[w].wait()
        own_down(0, w)

    @pl.when(plane == 1)
    def _():
        for copy in staged:
            copy.start()

    def open_plane():
        pltpu.make_async_copy(stage, stage, local.at[2]).wait()
        for w in (1, 0):
            for k in near:
                in_plane(k, w)
        for w in range(2):
            own_twin(0, w)

    @pl.when(plane == 0)
    def _():
        for device in beside:
            tell(met.at[0], device)

    @pl.when(plane == 2)
    def _():
        tell(met.at[1], down)

    @pl.when(plane != 1)
    def _():
        for w in range(2):
            own_up(0, w)
        open_plane()

    @pl.when(plane == 0)
    def _():
        pl.semaphore_wait(met.at[0], len(beside))
        tell(met.at[0], up)

    @pl.when(plane == 1)
    def _():
        pl.semaphore_wait(met.at[0], 1)
        open_plane()
        detour_down()
        pl.semaphore_wait(met.at[1], 1)
        for w in range(2):
            own_up(0, w)

    held = [caches.at[i] for i in range(2)]
    loads = [
        pltpu.make_async_copy(source, target, local.at[3 + i])
        for sources, targets, i in (
            ((old_qkv, old_out), [weights.at[:, pl.ds(sum(widths[:w]), widths[w])] for w in range(2)], 0),
            ((keys, values), held, 1),
        )
        for source, target in zip(sources, targets)
    ]
    for copy in loads + small:
        copy.start()
    arrivals = [(k, w) for w in (1, 0) for k in near] + [(k, w) for k in far for w in (1, 0)]
    for k, w in arrivals:
        landed(piece_rows(plane, core, k, w), a_recv.at[k - 1, w])
        own_down(k, w)
        own_up(k, w)
        own_twin(k, w)
        if (k, w) == arrivals[0]:
            for j in far:
                for v in (1, 0):
                    in_plane(j, v)

    detour_across()
    for copy in small:
        copy.wait()
    seqs = hidden.shape[0]
    lane = lax.broadcasted_iota(jnp.int32, (1, HD), 1)
    for s in range(seqs):
        angles = lengths[s].astype(jnp.float32) * frequency[...]
        cosine[s : s + 1, :] = jnp.cos(angles)
        sine[s : s + 1, :] = jnp.where(lane < HD // 2, -jnp.sin(angles), jnp.sin(angles))
    tile = 128
    pltpu.make_async_copy(weights, weights, local.at[3]).wait()
    pltpu.make_async_copy(caches, caches, local.at[4]).wait()

    @pl.loop(0, widths[0] // tile)
    def _(i):
        at = pl.ds(pl.multiple_of(i * tile, tile), tile)
        joined[tp, :, at] = jnp.dot(
            hidden[...], weights[:, at], preferred_element_type=jnp.float32
        ).astype(joined.dtype)

    def send_all(ref, send, recv):
        for k in range(1, tps):
            remote(ref.at[tp], ref.at[tp], send, recv, peers[k - 1]).start()

    send_all(joined, local.at[0], x_recv.at[2])

    relay(1)

    landed(joined.at[pl.ds(0, tps - 1)], x_recv.at[2])

    group = HQ // KVH
    positions = caches.shape[2]
    per_slot = joined.shape[2] // HD
    inv_root = 1.0 / jnp.sqrt(jnp.float32(HD))

    def head(j):
        at = (j % per_slot) * HD
        return joined[j // per_slot, :, at : at + HD].astype(jnp.float32)

    def turn(v):
        swapped = jnp.concatenate([v[:, HD // 2 :], v[:, : HD // 2]], axis=1)
        return (v * cosine[...] + swapped * sine[...]).astype(jnp.bfloat16).astype(jnp.float32)

    rotated[...] = jnp.zeros_like(rotated)
    own_score[...] = jnp.zeros_like(own_score)
    own_value[...] = jnp.zeros_like(own_value)
    for kv in range(KVH):
        own_key = turn(head(HQ + kv))
        new_value = head(HQ + KVH + kv)
        for g in range(group):
            query = turn(head(kv * group + g))
            rotated[:, kv * PAD + g, :] = query
            score = jnp.sum(query * own_key, axis=1, keepdims=True) * inv_root
            own_score[:, kv * PAD + g, :] = jnp.broadcast_to(score, (seqs, HD))
            own_value[:, kv * PAD + g, :] = new_value

    @pl.loop(0, seqs)
    def _(s):
        place = lax.broadcasted_iota(jnp.int32, (1, positions), 1) + tp * positions
        is_live = place < lengths[s]
        for kv in range(KVH):
            at = slice(kv * HD, (kv + 1) * HD)
            lanes = slice(kv * PAD, (kv + 1) * PAD)
            query = rotated[s, lanes, :].astype(jnp.bfloat16)
            scores = lax.dot_general(
                query, caches[0, s, :, at], (((1,), (1,)), ((), ())),
                preferred_element_type=jnp.float32,
            ) * inv_root
            scores = jnp.where(is_live, scores, jnp.float32(-1e30))
            top = jnp.max(scores, axis=1, keepdims=True)
            shares = jnp.where(is_live, jnp.exp(scores - top), 0.0).astype(jnp.bfloat16)
            total = jnp.sum(shares.astype(jnp.float32), axis=1, keepdims=True)
            parts[tp, 0, s, lanes, :] = jnp.dot(
                shares, caches[1, s, :, at], preferred_element_type=jnp.float32
            )
            parts[tp, 1, s, lanes, :] = jnp.broadcast_to(top, (PAD, HD))
            parts[tp, 2, s, lanes, :] = jnp.broadcast_to(total, (PAD, HD))

    send_all(parts, local.at[1], x_recv.at[3])

    for d in range(2, planes - 1):
        relay(d)
    @pl.when((plane < 2) & carries)
    def _():
        sent(detour, local.at[6])

    @pl.when((plane == 1) | (plane == planes - 2))
    def _():
        settle_twin(block, 1)

    @pl.when((core == 1) & (plane == planes - 2))
    def _():
        send_tails(0, up)

    @pl.when((core == 1) & (plane == 1))
    def _():
        send_tails(planes - 1, down)


    landed(parts.at[pl.ds(0, tps - 1)], x_recv.at[3])

    @pl.loop(0, seqs)
    def _(s):
        mine = own_score[s]
        top = mine
        for t in range(tps):
            top = jnp.maximum(top, parts[t, 1, s])
        mine = jnp.exp(mine - top).astype(jnp.bfloat16).astype(jnp.float32)
        numerator, denominator = mine * own_value[s], mine
        for t in range(tps):
            scale = jnp.exp(parts[t, 1, s] - top)
            numerator = numerator + parts[t, 0, s] * scale
            denominator = denominator + parts[t, 2, s] * scale
        rotated[s] = numerator / denominator

    for j in range(HQ):
        row = (j // group) * PAD + j % group
        attended[:, j * HD : (j + 1) * HD] = rotated[:, row, :].astype(attended.dtype)

    @pl.loop(0, widths[1] // tile)
    def _(i):
        at = pl.ds(pl.multiple_of(i * tile, tile), tile)
        under = pl.ds(pl.multiple_of(widths[0] + i * tile, tile), tile)
        decoded[:, at] = jnp.dot(
            attended[...], weights[:, under], preferred_element_type=jnp.float32
        ).astype(decoded.dtype)

    sent(bytes_of(tps - 1), local.at[5])
    sent(joined.at[pl.ds(0, tps - 1)], local.at[0])
    sent(parts.at[pl.ds(0, tps - 1)], local.at[1])
    settle_twin((planes - 1) * block, 0)
    settle_next(0)
    settle_next(planes - 1)
    at_end = (plane == 0) | (plane == planes - 1)
    relay(planes - 1)

    @pl.when((core == 1) & (plane == planes - 1))
    def _():
        take_tails(0)

    @pl.when((core == 1) & (plane == 0))
    def _():
        take_tails(planes - 1)

    @pl.when(at_end)
    def _():
        settle_twin(block - tail, 1)

    @pl.when(at_end & (core == 0))
    def _():
        landed(out_rows(2 * tail), t_recv.at[len(tails)])

    for p in range(1, planes - 1):
        settle_next(p)

    @pl.when((core == 1) & (at_end | (plane == 1) | (plane == planes - 2)))
    def _():
        sent(out_rows(2 * tail), local.at[6])


def flush_kernel(decoded, qkv, out, decoded_to, qkv_to, out_to, sems):
    pairs = ((decoded, decoded_to), (qkv, qkv_to), (out, out_to))
    for i, (source, target) in enumerate(pairs):
        cuts = max(c for c in range(1, CUTS + 1) if c == 1 or source.shape[0] % (16 * c) == 0)
        rows = source.shape[0] // cuts
        for j in range(cuts):
            at = pl.ds(j * rows, rows)
            pltpu.make_async_copy(source.at[at], target.at[at], sems.at[i]).start()
    for i, (source, target) in enumerate(pairs):
        pltpu.make_async_copy(source, target, sems.at[i]).wait()


def flush(*arrays):
    return pl.pallas_call(
        flush_kernel,
        out_shape=[jax.ShapeDtypeStruct(x.shape, x.dtype) for x in arrays],
        in_specs=[pl.BlockSpec(memory_space=pltpu.VMEM)] * 3,
        out_specs=[pl.BlockSpec(memory_space=pltpu.HBM)] * 3,
        scratch_shapes=[pltpu.SemaphoreType.DMA((3,))],
        compiler_params=pltpu.CompilerParams(vmem_limit_bytes=2**20),
    )(*arrays)


def fused(mesh, hidden, lengths, old_qkv, old_out, keys, values, new_qkv, new_out):
    reps, tps = mesh.shape["rep"], mesh.shape["tp"]
    planes = reps // 2
    seqs = keys.shape[0]
    rows = new_qkv.shape[0]
    widths = (new_qkv.shape[1] // tps, new_out.shape[1] // tps)
    half = HD // 2
    frequency = ROPE_BASE ** (-2.0 * np.arange(half) / (2 * half))
    frequency = jnp.asarray(np.concatenate([frequency, frequency])[None], jnp.float32)

    sem = pltpu.SemaphoreType.DMA
    whole, anywhere = pl.BlockSpec(memory_space=pltpu.VMEM), pl.BlockSpec(memory_space=pl.ANY)
    in_hbm = pl.BlockSpec(memory_space=pltpu.HBM)
    f32, bf16 = jnp.float32, jnp.bfloat16
    padded = KVH * PAD
    landed = 2 * rows * reps * tps * sum(widths)
    scratch = [sem((tps - 1, 2)), sem((2,)), sem((planes - 1, tps // 2)), sem((2,)), sem((2,))]
    scratch += [sem((5,)), sem((4,)), sem((7,)), pltpu.SemaphoreType.REGULAR((2,))]
    scratch += [pltpu.VMEM((rows, new_qkv.shape[1] + new_out.shape[1]), bf16)]
    scratch += [pltpu.VMEM((DETOUR, widths[1]), bf16)]
    scratch += [pltpu.VMEM((old_qkv.shape[0], sum(widths)), bf16), pltpu.VMEM((2, *keys.shape), bf16)]
    scratch += [
        pltpu.VMEM((tps, seqs, widths[0]), bf16),
        pltpu.VMEM((seqs, padded, HD), f32),
        pltpu.VMEM((seqs, padded, HD), f32),
        pltpu.VMEM((seqs, padded, HD), f32),
        pltpu.VMEM((tps, 3, seqs, padded, HD), f32),
        pltpu.VMEM((seqs, HQ * HD), bf16),
        pltpu.VMEM((seqs, HD), f32),
        pltpu.VMEM((seqs, HD), f32),
        pltpu.VMEM(hidden.shape, hidden.dtype),
        pltpu.VMEM(frequency.shape, frequency.dtype),
        pltpu.SMEM(lengths.shape, lengths.dtype),
    ]
    return pl.pallas_call(
        functools.partial(step_kernel, planes, tps),
        out_shape=[pltpu.VMEM((seqs, widths[1]), bf16)]
        + [pltpu.VMEM((rows * reps * tps, width), bf16) for width in widths],
        in_specs=[in_hbm] * 9,
        out_specs=[whole] + [anywhere] * 2,
        scratch_shapes=scratch,
        compiler_params=pltpu.CompilerParams(
            collective_id=0, has_side_effects=True, vmem_limit_bytes=VMEM_BYTES - landed - SLACK
        ),
    )(hidden, lengths, frequency, old_qkv, old_out, keys, values, new_qkv, new_out)


def solution(mesh):
    in_specs = (
        P("rep", None),
        P("rep"),
        P(None, "tp"),
        P(None, "tp"),
        P("rep", "tp", None),
        P("rep", "tp", None),
        P(("rep", "tp"), None),
        P(("rep", "tp"), None),
    )
    out_specs = (P("rep", "tp"), P(None, "tp"), P(None, "tp"))

    def step(*args):
        reps, tps = mesh.shape["rep"], mesh.shape["tp"]
        widths = [x.shape[1] // tps for x in args[6:]]
        rows = args[6].shape[0]
        tiled = rows % 16 == 0 and all(width % 128 == 0 for width in widths)
        tiled = tiled and rows > max(TAIL * 8, DETOUR) and rows * tps * sum(widths) % widths[1] == 0
        tiled = tiled and args[2].shape[0] == args[3].shape[0]
        if reps % 4 or reps < 6 or tps != 4 or not tiled:
            return (per_device(*args[:6]), *native_move(*args[6:]))
        return tuple(flush(*fused(mesh, *args)))

    return jax.shard_map(
        step, mesh=mesh, in_specs=in_specs, out_specs=out_specs, check_vma=False
    )
```

```python
import functools

import jax
import jax.numpy as jnp
import numpy as np
from jax import lax
from jax.experimental import pallas as pl
from jax.experimental.pallas import tpu as pltpu
from jax.sharding import PartitionSpec as P

HQ = 28
KVH = 4
HD = 128
PAD = 8
CUTS = 56
TAIL = 4
DETOUR = 16
VMEM_BYTES = 67043328
SLACK = 600000
MESH = pl.DeviceIdType.MESH


ROPE_BASE = 1000000.0


def rotate(vectors, positions):
    half_dim = vectors.shape[-1] // 2
    frequency = ROPE_BASE ** (-2.0 * jnp.arange(half_dim, dtype=jnp.float32) / (2 * half_dim))
    angles = positions.astype(jnp.float32)[:, None, None] * frequency
    first_half = vectors[..., :half_dim]
    second_half = vectors[..., half_dim:]
    return jnp.concatenate(
        [
            first_half * jnp.cos(angles) - second_half * jnp.sin(angles),
            second_half * jnp.cos(angles) + first_half * jnp.sin(angles),
        ],
        axis=-1,
    )


def per_device(hidden_state, lengths, old_qkv, old_out, cache_keys, cache_values):
    seq_count = hidden_state.shape[0]
    local_joined = jnp.dot(hidden_state, old_qkv, preferred_element_type=jnp.float32).astype(
        jnp.bfloat16
    )
    joined_rows = lax.all_gather(local_joined, "tp", axis=1, tiled=True)
    q_width = HQ * HD
    k_width = KVH * HD
    group_size = HQ // KVH
    queries = rotate(
        joined_rows[:, :q_width].astype(jnp.float32).reshape(seq_count, HQ, HD), lengths
    ).astype(jnp.bfloat16)
    own_keys = rotate(
        joined_rows[:, q_width : q_width + k_width].astype(jnp.float32).reshape(seq_count, KVH, HD),
        lengths,
    ).astype(jnp.bfloat16)
    own_values = joined_rows[:, q_width + k_width :].reshape(seq_count, KVH, HD)
    inv_root = 1.0 / jnp.sqrt(jnp.float32(HD))
    cache_rows = cache_keys.shape[1]
    grouped = queries.reshape(seq_count, KVH, group_size, HD)
    key_blocks = cache_keys.reshape(seq_count, cache_rows, KVH, HD)
    value_blocks = cache_values.reshape(seq_count, cache_rows, KVH, HD)
    scores = (
        jnp.einsum("skgd,stkd->skgt", grouped, key_blocks, preferred_element_type=jnp.float32)
        * inv_root
    )
    positions = lax.axis_index("tp") * cache_rows + jnp.arange(cache_rows, dtype=jnp.int32)
    live_mask = (positions[None, :] < lengths[:, None])[:, None, None, :]
    scores = jnp.where(live_mask, scores, jnp.float32(-1e30))
    own_score = (
        jnp.sum(grouped.astype(jnp.float32) * own_keys.astype(jnp.float32)[:, :, None, :], axis=-1)
        * inv_root
    )
    local_top = jnp.maximum(jnp.max(scores, axis=-1), own_score)
    top_score = lax.pmax(local_top, "tp")
    weights = jnp.where(live_mask, jnp.exp(scores - top_score[..., None]), jnp.float32(0.0)).astype(
        jnp.bfloat16
    )
    numer_part = jnp.einsum(
        "skgt,stkd->skgd", weights, value_blocks, preferred_element_type=jnp.float32
    )
    denom_part = jnp.sum(weights.astype(jnp.float32), axis=-1)
    numerator, denominator = lax.psum((numer_part, denom_part), "tp")
    own_weight = lax.optimization_barrier(
        jnp.exp(own_score - top_score).astype(jnp.bfloat16)
    ).astype(jnp.float32)
    numerator = numerator + own_weight[..., None] * own_values.astype(jnp.float32)[:, :, None, :]
    denominator = denominator + own_weight
    attended = (numerator / denominator[..., None]).reshape(seq_count, q_width).astype(jnp.bfloat16)
    decoded = jnp.dot(attended, old_out, preferred_element_type=jnp.float32).astype(jnp.bfloat16)
    return decoded


def native_move(new_qkv, new_out):
    def move(block):
        piece = lax.all_to_all(block, "tp", split_axis=1, concat_axis=0, tiled=True)
        return lax.all_gather(piece, "rep", axis=0, tiled=True)

    return move(new_qkv), move(new_out)


def flip(index, bits, size):
    out = index
    bit = 1
    while bit < size:
        if (bits // bit) % 2:
            out = out + bit - 2 * bit * ((index // bit) % 2)
        bit *= 2
    return out


def step_kernel(
    planes, tps,
    hidden_in, lengths_in, frequency_in, old_qkv, old_out, keys, values, new_qkv, new_out,
    decoded, qkv_full, out_full,
    a_recv, z_send, z_recv, s_send, s_recv, t_recv, x_recv, local, met,
    stage, detour,
    weights, caches, joined, rotated, own_score, own_value, parts, attended,
    cosine, sine, hidden, frequency, lengths,
):
    rep, tp = lax.axis_index("rep"), lax.axis_index("tp")
    plane, core = rep // 2, rep % 2
    rows = new_qkv.shape[0]
    fulls = (qkv_full, out_full)
    widths = (qkv_full.shape[1], out_full.shape[1])
    bases = (0, new_qkv.shape[1])
    up = (jnp.minimum(plane + 1, planes - 1) * 2 + core, tp)
    down = (jnp.maximum(plane - 1, 0) * 2 + core, tp)
    twin = (plane * 2 + 1 - core, tp)
    peers = [(rep, flip(tp, k, tps)) for k in range(1, tps)]
    near = [k for k in range(1, tps) if k & (k - 1) == 0]
    far = [k for k in range(1, tps) if k & (k - 1)]
    can_up, can_down = plane < planes - 1, plane > 0

    half = tps // 2

    def at_rows(source_plane, source_core, first, count, w):
        start = ((source_plane * 2 + source_core) * tps) * rows + first
        return fulls[w].at[pl.ds(pl.multiple_of(start, 16), count)]

    def piece_rows(source_plane, source_core, k, w):
        return at_rows(source_plane, source_core, flip(tp, k, tps) * rows, rows, w)

    mine = [
        pltpu.make_async_copy(
            source.at[:, pl.ds(pl.multiple_of(tp * widths[w], 128), widths[w])],
            piece_rows(plane, core, 0, w), local.at[w],
        )
        for w, source in enumerate((new_qkv, new_out))
    ]
    staged = [
        pltpu.make_async_copy(
            source, stage.at[:, pl.ds(bases[w], source.shape[1])], local.at[2]
        )
        for w, source in enumerate((new_qkv, new_out))
    ]
    barrier = pltpu.get_barrier_semaphore()
    beside = [twin] + [peers[k - 1] for k in near]

    def tell(semaphore, device):
        pl.semaphore_signal(semaphore, inc=1, device_id=device, device_id_type=MESH)

    @pl.when(can_up)
    def _():
        tell(barrier, up)

    @pl.when(can_down & (plane != 2))
    def _():
        tell(barrier, down)

    @pl.when(plane != 1)
    def _():
        for device in beside:
            tell(barrier, device)
        for copy in mine + staged:
            copy.start()

    small = [
        pltpu.make_async_copy(source, target, local.at[i])
        for i, (source, target) in enumerate(
            ((hidden_in, hidden), (frequency_in, frequency), (lengths_in, lengths))
        )
    ]

    @pl.when(plane == 1)
    def _():
        pl.semaphore_wait(barrier, 1)

    @pl.when((plane != 1) & can_up & can_down)
    def _():
        pl.semaphore_wait(barrier, len(beside) + 2)

    @pl.when(jnp.logical_not(can_up & can_down))
    def _():
        pl.semaphore_wait(barrier, len(beside) + 1)

    def remote(source, target, send, recv, device):
        return pltpu.make_async_remote_copy(
            src_ref=source, dst_ref=target, send_sem=send, recv_sem=recv,
            device_id=device, device_id_type=MESH,
        )

    def sent(ref, sem):
        remote(ref, ref, sem, sem, twin).wait_send()

    def landed(ref, sem):
        remote(ref, ref, sem, sem, twin).wait_recv()

    def pair_first(h):
        return (flip(tp, 2 * h, tps) // 2) * 2 * rows

    tail = TAIL * 16
    tails = [(1, first, count) for first, count in ((2 * rows - tail, tail - 16), (2 * rows - 16, 16))]
    tails = [(c, part) for part in tails for c in (1, 0)]

    def parts_of(h, last):
        if last and h == half - 1:
            return [(0, 0, 2 * rows, 0), (1, 0, 2 * rows - tail, 1)]
        return [(w, 0, 2 * rows, 0) for w in range(2)]

    def part_rows(source_plane, source_core, h, part):
        w, first, count = part[:3]
        return at_rows(source_plane, source_core, pair_first(h) + first, count, w)

    def part_sem(index, h, part):
        return x_recv.at[0] if part[3] else z_recv.at[index, h]

    def bytes_of(parts):
        return stage.at[:, pl.ds(0, stage.shape[1] // tps * parts)]

    def out_rows(count):
        return out_full.at[pl.ds(0, count)]

    def send_tails(source_plane, device):
        for i, (c, part) in enumerate(tails):
            ref = part_rows(source_plane, c, half - 1, part)
            remote(ref, ref, local.at[6], t_recv.at[i], device).start()

    def take_tails(source_plane):
        for i, (c, part) in enumerate(tails):
            ref = part_rows(source_plane, c, half - 1, part)
            landed(ref, t_recv.at[i])
            remote(ref, ref, local.at[6], t_recv.at[len(tails)], twin).start()

    def column(w, t):
        start = bases[w] + t * widths[w]
        return stage.at[:, pl.ds(pl.multiple_of(start, 128), widths[w])]

    def in_plane(k, w):
        remote(
            column(w, flip(tp, k, tps)), piece_rows(plane, core, 0, w),
            local.at[5], a_recv.at[k - 1, w], peers[k - 1],
        ).start()

    def own_up(k, w):
        ref = piece_rows(plane, core, k, w)

        @pl.when(can_up)
        def _():
            remote(ref, ref, z_send.at[0], z_recv.at[plane, k // 2], up).start()

    def own_down(k, w):
        ref = piece_rows(plane, core, k, w)

        def send(ref):
            remote(ref, ref, z_send.at[1], z_recv.at[plane - 1, k // 2], down).start()

        if w and k:
            short = detoured & (core == (k + 1) % 2)

            @pl.when(short)
            def _():
                send(at_rows(plane, core, flip(tp, k, tps) * rows, rows - DETOUR, w))

            @pl.when(can_down & jnp.logical_not(short))
            def _():
                send(ref)

        else:

            @pl.when(can_down)
            def _():
                send(ref)

    def own_twin(k, w):
        ref = piece_rows(plane, core, k, w)
        remote(ref, ref, s_send.at[0], s_recv.at[0], twin).start()

    detoured = (plane == 1) & (tp == 0)
    carries = (tp != 0) & (core == (tp + 1) % 2)

    def detour_down():
        @pl.when((plane == 1) & carries)
        def _():
            source = stage.at[pl.ds(rows - DETOUR, DETOUR), pl.ds(bases[1], widths[1])]
            remote(source, detour, local.at[6], x_recv.at[1], down).start()

    def detour_across():
        @pl.when((plane == 0) & carries)
        def _():
            landed(detour, x_recv.at[1])
            target = at_rows(1, core, tp * rows + rows - DETOUR, DETOUR, 1)
            remote(detour, target, local.at[6], z_recv.at[0, tp // 2], (rep, jnp.int32(0))).start()

    def take(source_plane, index, h, single, parts, far, can, device, way, onward):
        if single:
            (part,) = parts
            landed(part_rows(source_plane, core, h, part), part_sem(index, h, part))
        else:
            landed(bytes_of(2), z_recv.at[index, h])
        if onward:

            @pl.when(can)
            def _():
                for part in onward:
                    ref = part_rows(source_plane, core, h, part)
                    sem = part_sem(source_plane - way, h, part)
                    remote(ref, ref, z_send.at[way], sem, device).start()

        for part in parts:
            ref = part_rows(source_plane, core, h, part)
            remote(ref, ref, s_send.at[far], s_recv.at[far], twin).start()

    def farthest(source_plane):
        other = jnp.where(plane < planes // 2, planes - 1, 0)
        return jnp.where(source_plane == other, 1, 0)

    def relay(d):
        ends = d == planes - 1
        for h in range(half):
            cuts = parts_of(h, ends)
            onward = [] if ends else parts_of(h, d == planes - 2)
            single = ends and h == half - 1
            for parts in [[part] for part in cuts] if single else [cuts]:

                @pl.when(plane >= d)
                def _():
                    s = plane - d
                    take(s, s, h, single, parts, farthest(s), can_up, up, 0, onward)

                @pl.when(plane + d < planes)
                def _():
                    s = plane + d
                    take(s, s - 1, h, single, parts, farthest(s), can_down, down, 1, onward)

    block = rows * tps * sum(widths) // widths[1]

    def settle_twin(count, far):
        landed(out_rows(count), s_recv.at[far])
        sent(out_rows(count), s_send.at[far])

    def settle_next(p):
        @pl.when(plane == p)
        def _():
            for way, count in ((0, p + 1), (1, planes - p)):
                if p == (planes - 1, 0)[way]:
                    continue
                total = count * block - (tail if p == (planes - 2, 1)[way] else 0)
                if p != 1 or way == 0:
                    sent(out_rows(total), z_send.at[way])
                    continue

                @pl.when(tp != 0)
                def _():
                    sent(out_rows(total), z_send.at[way])

                for c in range(2):
                    cut = DETOUR * sum((k + 1) % 2 == c for k in range(1, tps))

                    @pl.when((tp == 0) & (core == c))
                    def _():
                        sent(out_rows(total - cut), z_send.at[way])

    @pl.when(plane == 1)
    def _():
        for w, source in enumerate((new_qkv, new_out)):
            columns = pl.ds(pl.multiple_of(tp * widths[w], 128), widths[w])
            remote(
                source.at[:, columns], piece_rows(plane, core, 0, w),
                z_send.at[1], z_recv.at[plane - 1, 0], down,
            ).start()
        for copy in mine + staged:
            copy.start()

    for w in range(2):
        mine[w].wait()

        @pl.when(plane != 1)
        def _():
            own_down(0, w)

    def open_plane():
        pltpu.make_async_copy(stage, stage, local.at[2]).wait()
        for w in (1, 0):
            for k in near:
                in_plane(k, w)
        for w in range(2):
            own_twin(0, w)

    @pl.when(plane == 0)
    def _():
        for device in beside:
            tell(met.at[0], device)

    @pl.when(plane == 2)
    def _():
        tell(met.at[1], down)

    @pl.when(plane != 1)
    def _():
        for w in range(2):
            own_up(0, w)
        open_plane()

    @pl.when(plane == 0)
    def _():
        pl.semaphore_wait(met.at[0], len(beside))
        tell(met.at[0], up)

    @pl.when(plane == 1)
    def _():
        pl.semaphore_wait(met.at[0], 1)
        open_plane()
        detour_down()
        pl.semaphore_wait(met.at[1], 1)
        for w in range(2):
            own_up(0, w)

    held = [caches.at[i] for i in range(2)]
    loads = [
        pltpu.make_async_copy(source, target, local.at[3 + i])
        for sources, targets, i in (
            ((old_qkv, old_out), [weights.at[:, pl.ds(sum(widths[:w]), widths[w])] for w in range(2)], 0),
            ((keys, values), held, 1),
        )
        for source, target in zip(sources, targets)
    ]
    for copy in loads + small:
        copy.start()
    arrivals = [(k, w) for w in (1, 0) for k in near] + [(k, w) for k in far for w in (1, 0)]
    for k, w in arrivals:
        landed(piece_rows(plane, core, k, w), a_recv.at[k - 1, w])
        own_down(k, w)
        own_up(k, w)
        own_twin(k, w)
        if (k, w) == arrivals[0]:
            for j in far:
                for v in (1, 0):
                    in_plane(j, v)

    detour_across()
    for copy in small:
        copy.wait()
    seqs = hidden.shape[0]
    lane = lax.broadcasted_iota(jnp.int32, (1, HD), 1)
    for s in range(seqs):
        angles = lengths[s].astype(jnp.float32) * frequency[...]
        cosine[s : s + 1, :] = jnp.cos(angles)
        sine[s : s + 1, :] = jnp.where(lane < HD // 2, -jnp.sin(angles), jnp.sin(angles))
    tile = 128
    pltpu.make_async_copy(weights, weights, local.at[3]).wait()
    pltpu.make_async_copy(caches, caches, local.at[4]).wait()

    @pl.loop(0, widths[0] // tile)
    def _(i):
        at = pl.ds(pl.multiple_of(i * tile, tile), tile)
        joined[tp, :, at] = jnp.dot(
            hidden[...], weights[:, at], preferred_element_type=jnp.float32
        ).astype(joined.dtype)

    def send_all(ref, send, recv):
        for k in range(1, tps):
            remote(ref.at[tp], ref.at[tp], send, recv, peers[k - 1]).start()

    send_all(joined, local.at[0], x_recv.at[2])

    relay(1)

    landed(joined.at[pl.ds(0, tps - 1)], x_recv.at[2])

    group = HQ // KVH
    positions = caches.shape[2]
    per_slot = joined.shape[2] // HD
    inv_root = 1.0 / jnp.sqrt(jnp.float32(HD))

    def head(j):
        at = (j % per_slot) * HD
        return joined[j // per_slot, :, at : at + HD].astype(jnp.float32)

    def turn(v):
        swapped = jnp.concatenate([v[:, HD // 2 :], v[:, : HD // 2]], axis=1)
        return (v * cosine[...] + swapped * sine[...]).astype(jnp.bfloat16).astype(jnp.float32)

    rotated[...] = jnp.zeros_like(rotated)
    own_score[...] = jnp.zeros_like(own_score)
    own_value[...] = jnp.zeros_like(own_value)
    for kv in range(KVH):
        own_key = turn(head(HQ + kv))
        new_value = head(HQ + KVH + kv)
        for g in range(group):
            query = turn(head(kv * group + g))
            rotated[:, kv * PAD + g, :] = query
            score = jnp.sum(query * own_key, axis=1, keepdims=True) * inv_root
            own_score[:, kv * PAD + g, :] = jnp.broadcast_to(score, (seqs, HD))
            own_value[:, kv * PAD + g, :] = new_value

    @pl.loop(0, seqs)
    def _(s):
        place = lax.broadcasted_iota(jnp.int32, (1, positions), 1) + tp * positions
        is_live = place < lengths[s]
        for kv in range(KVH):
            at = slice(kv * HD, (kv + 1) * HD)
            lanes = slice(kv * PAD, (kv + 1) * PAD)
            query = rotated[s, lanes, :].astype(jnp.bfloat16)
            scores = lax.dot_general(
                query, caches[0, s, :, at], (((1,), (1,)), ((), ())),
                preferred_element_type=jnp.float32,
            ) * inv_root
            scores = jnp.where(is_live, scores, jnp.float32(-1e30))
            top = jnp.max(scores, axis=1, keepdims=True)
            shares = jnp.where(is_live, jnp.exp(scores - top), 0.0).astype(jnp.bfloat16)
            total = jnp.sum(shares.astype(jnp.float32), axis=1, keepdims=True)
            parts[tp, 0, s, lanes, :] = jnp.dot(
                shares, caches[1, s, :, at], preferred_element_type=jnp.float32
            )
            parts[tp, 1, s, lanes, :] = jnp.broadcast_to(top, (PAD, HD))
            parts[tp, 2, s, lanes, :] = jnp.broadcast_to(total, (PAD, HD))

    send_all(parts, local.at[1], x_recv.at[3])

    for d in range(2, planes - 1):
        relay(d)
    @pl.when((plane < 2) & carries)
    def _():
        sent(detour, local.at[6])

    @pl.when((plane == 1) | (plane == planes - 2))
    def _():
        settle_twin(block, 1)

    @pl.when((core == 1) & (plane == planes - 2))
    def _():
        send_tails(0, up)

    @pl.when((core == 1) & (plane == 1))
    def _():
        send_tails(planes - 1, down)


    landed(parts.at[pl.ds(0, tps - 1)], x_recv.at[3])

    @pl.loop(0, seqs)
    def _(s):
        mine = own_score[s]
        top = mine
        for t in range(tps):
            top = jnp.maximum(top, parts[t, 1, s])
        mine = jnp.exp(mine - top).astype(jnp.bfloat16).astype(jnp.float32)
        numerator, denominator = mine * own_value[s], mine
        for t in range(tps):
            scale = jnp.exp(parts[t, 1, s] - top)
            numerator = numerator + parts[t, 0, s] * scale
            denominator = denominator + parts[t, 2, s] * scale
        rotated[s] = numerator / denominator

    for j in range(HQ):
        row = (j // group) * PAD + j % group
        attended[:, j * HD : (j + 1) * HD] = rotated[:, row, :].astype(attended.dtype)

    @pl.loop(0, widths[1] // tile)
    def _(i):
        at = pl.ds(pl.multiple_of(i * tile, tile), tile)
        under = pl.ds(pl.multiple_of(widths[0] + i * tile, tile), tile)
        decoded[:, at] = jnp.dot(
            attended[...], weights[:, under], preferred_element_type=jnp.float32
        ).astype(decoded.dtype)

    sent(bytes_of(tps - 1), local.at[5])
    sent(joined.at[pl.ds(0, tps - 1)], local.at[0])
    sent(parts.at[pl.ds(0, tps - 1)], local.at[1])
    settle_twin((planes - 1) * block, 0)
    settle_next(0)
    settle_next(planes - 1)
    at_end = (plane == 0) | (plane == planes - 1)
    relay(planes - 1)

    @pl.when((core == 1) & (plane == planes - 1))
    def _():
        take_tails(0)

    @pl.when((core == 1) & (plane == 0))
    def _():
        take_tails(planes - 1)

    @pl.when(at_end)
    def _():
        settle_twin(block - tail, 1)

    @pl.when(at_end & (core == 0))
    def _():
        landed(out_rows(2 * tail), t_recv.at[len(tails)])

    for p in range(1, planes - 1):
        settle_next(p)

    @pl.when((core == 1) & (at_end | (plane == 1) | (plane == planes - 2)))
    def _():
        sent(out_rows(2 * tail), local.at[6])


def flush_kernel(decoded, qkv, out, decoded_to, qkv_to, out_to, sems):
    pairs = ((decoded, decoded_to), (qkv, qkv_to), (out, out_to))
    for i, (source, target) in enumerate(pairs):
        cuts = max(c for c in range(1, CUTS + 1) if c == 1 or source.shape[0] % (16 * c) == 0)
        rows = source.shape[0] // cuts
        for j in range(cuts):
            at = pl.ds(j * rows, rows)
            pltpu.make_async_copy(source.at[at], target.at[at], sems.at[i]).start()
    for i, (source, target) in enumerate(pairs):
        pltpu.make_async_copy(source, target, sems.at[i]).wait()


def flush(*arrays):
    return pl.pallas_call(
        flush_kernel,
        out_shape=[jax.ShapeDtypeStruct(x.shape, x.dtype) for x in arrays],
        in_specs=[pl.BlockSpec(memory_space=pltpu.VMEM)] * 3,
        out_specs=[pl.BlockSpec(memory_space=pltpu.HBM)] * 3,
        scratch_shapes=[pltpu.SemaphoreType.DMA((3,))],
        compiler_params=pltpu.CompilerParams(vmem_limit_bytes=2**20),
    )(*arrays)


def fused(mesh, hidden, lengths, old_qkv, old_out, keys, values, new_qkv, new_out):
    reps, tps = mesh.shape["rep"], mesh.shape["tp"]
    planes = reps // 2
    seqs = keys.shape[0]
    rows = new_qkv.shape[0]
    widths = (new_qkv.shape[1] // tps, new_out.shape[1] // tps)
    half = HD // 2
    frequency = ROPE_BASE ** (-2.0 * np.arange(half) / (2 * half))
    frequency = jnp.asarray(np.concatenate([frequency, frequency])[None], jnp.float32)

    sem = pltpu.SemaphoreType.DMA
    whole, anywhere = pl.BlockSpec(memory_space=pltpu.VMEM), pl.BlockSpec(memory_space=pl.ANY)
    in_hbm = pl.BlockSpec(memory_space=pltpu.HBM)
    f32, bf16 = jnp.float32, jnp.bfloat16
    padded = KVH * PAD
    landed = 2 * rows * reps * tps * sum(widths)
    scratch = [sem((tps - 1, 2)), sem((2,)), sem((planes - 1, tps // 2)), sem((2,)), sem((2,))]
    scratch += [sem((5,)), sem((4,)), sem((7,)), pltpu.SemaphoreType.REGULAR((2,))]
    scratch += [pltpu.VMEM((rows, new_qkv.shape[1] + new_out.shape[1]), bf16)]
    scratch += [pltpu.VMEM((DETOUR, widths[1]), bf16)]
    scratch += [pltpu.VMEM((old_qkv.shape[0], sum(widths)), bf16), pltpu.VMEM((2, *keys.shape), bf16)]
    scratch += [
        pltpu.VMEM((tps, seqs, widths[0]), bf16),
        pltpu.VMEM((seqs, padded, HD), f32),
        pltpu.VMEM((seqs, padded, HD), f32),
        pltpu.VMEM((seqs, padded, HD), f32),
        pltpu.VMEM((tps, 3, seqs, padded, HD), f32),
        pltpu.VMEM((seqs, HQ * HD), bf16),
        pltpu.VMEM((seqs, HD), f32),
        pltpu.VMEM((seqs, HD), f32),
        pltpu.VMEM(hidden.shape, hidden.dtype),
        pltpu.VMEM(frequency.shape, frequency.dtype),
        pltpu.SMEM(lengths.shape, lengths.dtype),
    ]
    return pl.pallas_call(
        functools.partial(step_kernel, planes, tps),
        out_shape=[pltpu.VMEM((seqs, widths[1]), bf16)]
        + [pltpu.VMEM((rows * reps * tps, width), bf16) for width in widths],
        in_specs=[in_hbm] * 9,
        out_specs=[whole] + [anywhere] * 2,
        scratch_shapes=scratch,
        compiler_params=pltpu.CompilerParams(
            collective_id=0, has_side_effects=True, vmem_limit_bytes=VMEM_BYTES - landed - SLACK
        ),
    )(hidden, lengths, frequency, old_qkv, old_out, keys, values, new_qkv, new_out)


def solution(mesh):
    in_specs = (
        P("rep", None),
        P("rep"),
        P(None, "tp"),
        P(None, "tp"),
        P("rep", "tp", None),
        P("rep", "tp", None),
        P(("rep", "tp"), None),
        P(("rep", "tp"), None),
    )
    out_specs = (P("rep", "tp"), P(None, "tp"), P(None, "tp"))

    def step(*args):
        reps, tps = mesh.shape["rep"], mesh.shape["tp"]
        widths = [x.shape[1] // tps for x in args[6:]]
        rows = args[6].shape[0]
        tiled = rows % 16 == 0 and all(width % 128 == 0 for width in widths)
        tiled = tiled and rows > max(TAIL * 8, DETOUR) and rows * tps * sum(widths) % widths[1] == 0
        tiled = tiled and args[2].shape[0] == args[3].shape[0]
        if reps % 4 or reps < 6 or tps != 4 or not tiled:
            return (per_device(*args[:6]), *native_move(*args[6:]))
        return tuple(flush(*fused(mesh, *args)))

    return jax.shard_map(
        step, mesh=mesh, in_specs=in_specs, out_specs=out_specs, check_vma=False
    )
```

```python
import functools

import jax
import jax.numpy as jnp
import numpy as np
from jax import lax
from jax.experimental import pallas as pl
from jax.experimental.pallas import tpu as pltpu
from jax.sharding import PartitionSpec as P

HQ = 28
KVH = 4
HD = 128
PAD = 8
CUTS = 56
TAIL = 4
DETOUR = 16
VMEM_BYTES = 67043328
SLACK = 600000
MESH = pl.DeviceIdType.MESH


ROPE_BASE = 1000000.0


def rotate(vectors, positions):
    half_dim = vectors.shape[-1] // 2
    frequency = ROPE_BASE ** (-2.0 * jnp.arange(half_dim, dtype=jnp.float32) / (2 * half_dim))
    angles = positions.astype(jnp.float32)[:, None, None] * frequency
    first_half = vectors[..., :half_dim]
    second_half = vectors[..., half_dim:]
    return jnp.concatenate(
        [
            first_half * jnp.cos(angles) - second_half * jnp.sin(angles),
            second_half * jnp.cos(angles) + first_half * jnp.sin(angles),
        ],
        axis=-1,
    )


def per_device(hidden_state, lengths, old_qkv, old_out, cache_keys, cache_values):
    seq_count = hidden_state.shape[0]
    local_joined = jnp.dot(hidden_state, old_qkv, preferred_element_type=jnp.float32).astype(
        jnp.bfloat16
    )
    joined_rows = lax.all_gather(local_joined, "tp", axis=1, tiled=True)
    q_width = HQ * HD
    k_width = KVH * HD
    group_size = HQ // KVH
    queries = rotate(
        joined_rows[:, :q_width].astype(jnp.float32).reshape(seq_count, HQ, HD), lengths
    ).astype(jnp.bfloat16)
    own_keys = rotate(
        joined_rows[:, q_width : q_width + k_width].astype(jnp.float32).reshape(seq_count, KVH, HD),
        lengths,
    ).astype(jnp.bfloat16)
    own_values = joined_rows[:, q_width + k_width :].reshape(seq_count, KVH, HD)
    inv_root = 1.0 / jnp.sqrt(jnp.float32(HD))
    cache_rows = cache_keys.shape[1]
    grouped = queries.reshape(seq_count, KVH, group_size, HD)
    key_blocks = cache_keys.reshape(seq_count, cache_rows, KVH, HD)
    value_blocks = cache_values.reshape(seq_count, cache_rows, KVH, HD)
    scores = (
        jnp.einsum("skgd,stkd->skgt", grouped, key_blocks, preferred_element_type=jnp.float32)
        * inv_root
    )
    positions = lax.axis_index("tp") * cache_rows + jnp.arange(cache_rows, dtype=jnp.int32)
    live_mask = (positions[None, :] < lengths[:, None])[:, None, None, :]
    scores = jnp.where(live_mask, scores, jnp.float32(-1e30))
    own_score = (
        jnp.sum(grouped.astype(jnp.float32) * own_keys.astype(jnp.float32)[:, :, None, :], axis=-1)
        * inv_root
    )
    local_top = jnp.maximum(jnp.max(scores, axis=-1), own_score)
    top_score = lax.pmax(local_top, "tp")
    weights = jnp.where(live_mask, jnp.exp(scores - top_score[..., None]), jnp.float32(0.0)).astype(
        jnp.bfloat16
    )
    numer_part = jnp.einsum(
        "skgt,stkd->skgd", weights, value_blocks, preferred_element_type=jnp.float32
    )
    denom_part = jnp.sum(weights.astype(jnp.float32), axis=-1)
    numerator, denominator = lax.psum((numer_part, denom_part), "tp")
    own_weight = lax.optimization_barrier(
        jnp.exp(own_score - top_score).astype(jnp.bfloat16)
    ).astype(jnp.float32)
    numerator = numerator + own_weight[..., None] * own_values.astype(jnp.float32)[:, :, None, :]
    denominator = denominator + own_weight
    attended = (numerator / denominator[..., None]).reshape(seq_count, q_width).astype(jnp.bfloat16)
    decoded = jnp.dot(attended, old_out, preferred_element_type=jnp.float32).astype(jnp.bfloat16)
    return decoded


def native_move(new_qkv, new_out):
    def move(block):
        piece = lax.all_to_all(block, "tp", split_axis=1, concat_axis=0, tiled=True)
        return lax.all_gather(piece, "rep", axis=0, tiled=True)

    return move(new_qkv), move(new_out)


def flip(index, bits, size):
    out = index
    bit = 1
    while bit < size:
        if (bits // bit) % 2:
            out = out + bit - 2 * bit * ((index // bit) % 2)
        bit *= 2
    return out


def step_kernel(
    planes, tps,
    hidden_in, lengths_in, frequency_in, old_qkv, old_out, keys, values, new_qkv, new_out,
    decoded, qkv_full, out_full,
    a_recv, z_send, z_recv, s_send, s_recv, t_recv, x_recv, local, met,
    stage, detour,
    weights, caches, joined, rotated, own_score, own_value, parts, attended,
    cosine, sine, hidden, frequency, lengths,
):
    rep, tp = lax.axis_index("rep"), lax.axis_index("tp")
    plane, core = rep // 2, rep % 2
    rows = new_qkv.shape[0]
    fulls = (qkv_full, out_full)
    widths = (qkv_full.shape[1], out_full.shape[1])
    bases = (0, new_qkv.shape[1])
    up = (jnp.minimum(plane + 1, planes - 1) * 2 + core, tp)
    down = (jnp.maximum(plane - 1, 0) * 2 + core, tp)
    twin = (plane * 2 + 1 - core, tp)
    peers = [(rep, flip(tp, k, tps)) for k in range(1, tps)]
    near = [k for k in range(1, tps) if k & (k - 1) == 0]
    far = [k for k in range(1, tps) if k & (k - 1)]
    can_up, can_down = plane < planes - 1, plane > 0

    half = tps // 2

    def at_rows(source_plane, source_core, first, count, w):
        start = ((source_plane * 2 + source_core) * tps) * rows + first
        return fulls[w].at[pl.ds(pl.multiple_of(start, 16), count)]

    def piece_rows(source_plane, source_core, k, w):
        return at_rows(source_plane, source_core, flip(tp, k, tps) * rows, rows, w)

    mine = [
        pltpu.make_async_copy(
            source.at[:, pl.ds(pl.multiple_of(tp * widths[w], 128), widths[w])],
            piece_rows(plane, core, 0, w), local.at[w],
        )
        for w, source in enumerate((new_qkv, new_out))
    ]
    staged = [
        pltpu.make_async_copy(
            source, stage.at[:, pl.ds(bases[w], source.shape[1])], local.at[2]
        )
        for w, source in enumerate((new_qkv, new_out))
    ]
    barrier = pltpu.get_barrier_semaphore()
    beside = [twin] + [peers[k - 1] for k in near]

    def tell(semaphore, device):
        pl.semaphore_signal(semaphore, inc=1, device_id=device, device_id_type=MESH)

    @pl.when(can_up)
    def _():
        tell(barrier, up)

    @pl.when(can_down & (plane != 2))
    def _():
        tell(barrier, down)

    @pl.when(plane != 1)
    def _():
        for device in beside:
            tell(barrier, device)
        for copy in mine + staged:
            copy.start()

    small = [
        pltpu.make_async_copy(source, target, local.at[i])
        for i, (source, target) in enumerate(
            ((hidden_in, hidden), (frequency_in, frequency), (lengths_in, lengths))
        )
    ]

    @pl.when(plane == 1)
    def _():
        pl.semaphore_wait(barrier, 1)

    @pl.when((plane != 1) & can_up & can_down)
    def _():
        pl.semaphore_wait(barrier, len(beside) + 2)

    @pl.when(jnp.logical_not(can_up & can_down))
    def _():
        pl.semaphore_wait(barrier, len(beside) + 1)

    def remote(source, target, send, recv, device):
        return pltpu.make_async_remote_copy(
            src_ref=source, dst_ref=target, send_sem=send, recv_sem=recv,
            device_id=device, device_id_type=MESH,
        )

    def sent(ref, sem):
        remote(ref, ref, sem, sem, twin).wait_send()

    def landed(ref, sem):
        remote(ref, ref, sem, sem, twin).wait_recv()

    def pair_first(h):
        return (flip(tp, 2 * h, tps) // 2) * 2 * rows

    tail = TAIL * 16
    tails = [(1, first, count) for first, count in ((2 * rows - tail, tail - 16), (2 * rows - 16, 16))]
    tails = [(c, part) for part in tails for c in (1, 0)]

    def parts_of(h, last):
        if last and h == half - 1:
            return [(0, 0, 2 * rows, 0), (1, 0, 2 * rows - tail, 1)]
        return [(w, 0, 2 * rows, 0) for w in range(2)]

    def part_rows(source_plane, source_core, h, part):
        w, first, count = part[:3]
        return at_rows(source_plane, source_core, pair_first(h) + first, count, w)

    def part_sem(index, h, part):
        return x_recv.at[0] if part[3] else z_recv.at[index, h]

    def bytes_of(parts):
        return stage.at[:, pl.ds(0, stage.shape[1] // tps * parts)]

    def out_rows(count):
        return out_full.at[pl.ds(0, count)]

    def send_tails(source_plane, device):
        for i, (c, part) in enumerate(tails):
            ref = part_rows(source_plane, c, half - 1, part)
            if i == len(tails) - 1:
                other = (device[0] - 1, tp)
                remote(ref, ref, local.at[6], t_recv.at[len(tails)], other).start()
            remote(ref, ref, local.at[6], t_recv.at[i], device).start()

    def take_tails(source_plane):
        for i, (c, part) in enumerate(tails):
            ref = part_rows(source_plane, c, half - 1, part)
            landed(ref, t_recv.at[i])
            if i < len(tails) - 1:
                remote(ref, ref, local.at[6], t_recv.at[len(tails)], twin).start()

    def column(w, t):
        start = bases[w] + t * widths[w]
        return stage.at[:, pl.ds(pl.multiple_of(start, 128), widths[w])]

    def in_plane(k, w):
        remote(
            column(w, flip(tp, k, tps)), piece_rows(plane, core, 0, w),
            local.at[5], a_recv.at[k - 1, w], peers[k - 1],
        ).start()

    def own_up(k, w):
        ref = piece_rows(plane, core, k, w)

        @pl.when(can_up)
        def _():
            remote(ref, ref, z_send.at[0], z_recv.at[plane, k // 2], up).start()

    def own_down(k, w):
        ref = piece_rows(plane, core, k, w)

        def send(ref):
            remote(ref, ref, z_send.at[1], z_recv.at[plane - 1, k // 2], down).start()

        if w and k:
            short = detoured & (core == (k + 1) % 2)

            @pl.when(short)
            def _():
                send(at_rows(plane, core, flip(tp, k, tps) * rows, rows - DETOUR, w))

            @pl.when(can_down & jnp.logical_not(short))
            def _():
                send(ref)

        else:

            @pl.when(can_down)
            def _():
                send(ref)

    def own_twin(k, w):
        ref = piece_rows(plane, core, k, w)
        remote(ref, ref, s_send.at[0], s_recv.at[0], twin).start()

    detoured = (plane == 1) & (tp == 0)
    carries = (tp != 0) & (core == (tp + 1) % 2)

    def detour_down():
        @pl.when((plane == 1) & carries)
        def _():
            source = stage.at[pl.ds(rows - DETOUR, DETOUR), pl.ds(bases[1], widths[1])]
            remote(source, detour, local.at[6], x_recv.at[1], down).start()

    def detour_across():
        @pl.when((plane == 0) & carries)
        def _():
            landed(detour, x_recv.at[1])
            target = at_rows(1, core, tp * rows + rows - DETOUR, DETOUR, 1)
            remote(detour, target, local.at[6], z_recv.at[0, tp // 2], (rep, jnp.int32(0))).start()

    def take(source_plane, index, h, single, parts, far, can, device, way, onward):
        if single:
            (part,) = parts
            landed(part_rows(source_plane, core, h, part), part_sem(index, h, part))
        else:
            landed(bytes_of(2), z_recv.at[index, h])
        if onward:

            @pl.when(can)
            def _():
                for part in onward:
                    ref = part_rows(source_plane, core, h, part)
                    sem = part_sem(source_plane - way, h, part)
                    remote(ref, ref, z_send.at[way], sem, device).start()

        for part in parts:
            ref = part_rows(source_plane, core, h, part)
            remote(ref, ref, s_send.at[far], s_recv.at[far], twin).start()

    def farthest(source_plane):
        other = jnp.where(plane < planes // 2, planes - 1, 0)
        return jnp.where(source_plane == other, 1, 0)

    def relay(d):
        ends = d == planes - 1
        for h in range(half):
            cuts = parts_of(h, ends)
            onward = [] if ends else parts_of(h, d == planes - 2)
            single = ends and h == half - 1
            for parts in [[part] for part in cuts] if single else [cuts]:

                @pl.when(plane >= d)
                def _():
                    s = plane - d
                    take(s, s, h, single, parts, farthest(s), can_up, up, 0, onward)

                @pl.when(plane + d < planes)
                def _():
                    s = plane + d
                    take(s, s - 1, h, single, parts, farthest(s), can_down, down, 1, onward)

    block = rows * tps * sum(widths) // widths[1]

    def settle_twin(count, far):
        landed(out_rows(count), s_recv.at[far])
        sent(out_rows(count), s_send.at[far])

    def settle_next(p):
        @pl.when(plane == p)
        def _():
            for way, count in ((0, p + 1), (1, planes - p)):
                if p == (planes - 1, 0)[way]:
                    continue
                total = count * block - (tail if p == (planes - 2, 1)[way] else 0)
                if p != 1 or way == 0:
                    sent(out_rows(total), z_send.at[way])
                    continue

                @pl.when(tp != 0)
                def _():
                    sent(out_rows(total), z_send.at[way])

                for c in range(2):
                    cut = DETOUR * sum((k + 1) % 2 == c for k in range(1, tps))

                    @pl.when((tp == 0) & (core == c))
                    def _():
                        sent(out_rows(total - cut), z_send.at[way])

    @pl.when(plane == 1)
    def _():
        for w, source in enumerate((new_qkv, new_out)):
            columns = pl.ds(pl.multiple_of(tp * widths[w], 128), widths[w])
            remote(
                source.at[:, columns], piece_rows(plane, core, 0, w),
                z_send.at[1], z_recv.at[plane - 1, 0], down,
            ).start()
        for copy in mine + staged:
            copy.start()

    for w in range(2):
        mine[w].wait()

        @pl.when(plane != 1)
        def _():
            own_down(0, w)

    def open_plane():
        pltpu.make_async_copy(stage, stage, local.at[2]).wait()
        for w in (1, 0):
            for k in near:
                in_plane(k, w)
        for w in range(2):
            own_twin(0, w)

    @pl.when(plane == 0)
    def _():
        for device in beside:
            tell(met.at[0], device)

    @pl.when(plane == 2)
    def _():
        tell(met.at[1], down)

    @pl.when(plane != 1)
    def _():
        for w in range(2):
            own_up(0, w)
        open_plane()

    @pl.when(plane == 0)
    def _():
        pl.semaphore_wait(met.at[0], len(beside))
        tell(met.at[0], up)

    @pl.when(plane == 1)
    def _():
        pl.semaphore_wait(met.at[0], 1)
        open_plane()
        detour_down()
        pl.semaphore_wait(met.at[1], 1)
        for w in range(2):
            own_up(0, w)

    held = [caches.at[i] for i in range(2)]
    loads = [
        pltpu.make_async_copy(source, target, local.at[3 + i])
        for sources, targets, i in (
            ((old_qkv, old_out), [weights.at[:, pl.ds(sum(widths[:w]), widths[w])] for w in range(2)], 0),
            ((keys, values), held, 1),
        )
        for source, target in zip(sources, targets)
    ]
    for copy in loads + small:
        copy.start()
    arrivals = [(k, w) for w in (1, 0) for k in near] + [(k, w) for k in far for w in (1, 0)]
    for k, w in arrivals:
        landed(piece_rows(plane, core, k, w), a_recv.at[k - 1, w])
        own_down(k, w)
        own_up(k, w)
        own_twin(k, w)
        if (k, w) == arrivals[0]:
            for j in far:
                for v in (1, 0):
                    in_plane(j, v)

    detour_across()
    for copy in small:
        copy.wait()
    seqs = hidden.shape[0]
    lane = lax.broadcasted_iota(jnp.int32, (1, HD), 1)
    for s in range(seqs):
        angles = lengths[s].astype(jnp.float32) * frequency[...]
        cosine[s : s + 1, :] = jnp.cos(angles)
        sine[s : s + 1, :] = jnp.where(lane < HD // 2, -jnp.sin(angles), jnp.sin(angles))
    tile = 128
    pltpu.make_async_copy(weights, weights, local.at[3]).wait()
    pltpu.make_async_copy(caches, caches, local.at[4]).wait()

    @pl.loop(0, widths[0] // tile)
    def _(i):
        at = pl.ds(pl.multiple_of(i * tile, tile), tile)
        joined[tp, :, at] = jnp.dot(
            hidden[...], weights[:, at], preferred_element_type=jnp.float32
        ).astype(joined.dtype)

    def send_all(ref, send, recv):
        for k in range(1, tps):
            remote(ref.at[tp], ref.at[tp], send, recv, peers[k - 1]).start()

    send_all(joined, local.at[0], x_recv.at[2])

    relay(1)

    landed(joined.at[pl.ds(0, tps - 1)], x_recv.at[2])

    group = HQ // KVH
    positions = caches.shape[2]
    per_slot = joined.shape[2] // HD
    inv_root = 1.0 / jnp.sqrt(jnp.float32(HD))

    def head(j):
        at = (j % per_slot) * HD
        return joined[j // per_slot, :, at : at + HD].astype(jnp.float32)

    def turn(v):
        swapped = jnp.concatenate([v[:, HD // 2 :], v[:, : HD // 2]], axis=1)
        return (v * cosine[...] + swapped * sine[...]).astype(jnp.bfloat16).astype(jnp.float32)

    rotated[...] = jnp.zeros_like(rotated)
    own_score[...] = jnp.zeros_like(own_score)
    own_value[...] = jnp.zeros_like(own_value)
    for kv in range(KVH):
        own_key = turn(head(HQ + kv))
        new_value = head(HQ + KVH + kv)
        for g in range(group):
            query = turn(head(kv * group + g))
            rotated[:, kv * PAD + g, :] = query
            score = jnp.sum(query * own_key, axis=1, keepdims=True) * inv_root
            own_score[:, kv * PAD + g, :] = jnp.broadcast_to(score, (seqs, HD))
            own_value[:, kv * PAD + g, :] = new_value

    @pl.loop(0, seqs)
    def _(s):
        place = lax.broadcasted_iota(jnp.int32, (1, positions), 1) + tp * positions
        is_live = place < lengths[s]
        for kv in range(KVH):
            at = slice(kv * HD, (kv + 1) * HD)
            lanes = slice(kv * PAD, (kv + 1) * PAD)
            query = rotated[s, lanes, :].astype(jnp.bfloat16)
            scores = lax.dot_general(
                query, caches[0, s, :, at], (((1,), (1,)), ((), ())),
                preferred_element_type=jnp.float32,
            ) * inv_root
            scores = jnp.where(is_live, scores, jnp.float32(-1e30))
            top = jnp.max(scores, axis=1, keepdims=True)
            shares = jnp.where(is_live, jnp.exp(scores - top), 0.0).astype(jnp.bfloat16)
            total = jnp.sum(shares.astype(jnp.float32), axis=1, keepdims=True)
            parts[tp, 0, s, lanes, :] = jnp.dot(
                shares, caches[1, s, :, at], preferred_element_type=jnp.float32
            )
            parts[tp, 1, s, lanes, :] = jnp.broadcast_to(top, (PAD, HD))
            parts[tp, 2, s, lanes, :] = jnp.broadcast_to(total, (PAD, HD))

    send_all(parts, local.at[1], x_recv.at[3])

    for d in range(2, planes - 1):
        relay(d)
    @pl.when((plane < 2) & carries)
    def _():
        sent(detour, local.at[6])

    @pl.when((plane == 1) | (plane == planes - 2))
    def _():
        settle_twin(block, 1)

    @pl.when((core == 1) & (plane == planes - 2))
    def _():
        send_tails(0, up)

    @pl.when((core == 1) & (plane == 1))
    def _():
        send_tails(planes - 1, down)


    landed(parts.at[pl.ds(0, tps - 1)], x_recv.at[3])

    @pl.loop(0, seqs)
    def _(s):
        mine = own_score[s]
        top = mine
        for t in range(tps):
            top = jnp.maximum(top, parts[t, 1, s])
        mine = jnp.exp(mine - top).astype(jnp.bfloat16).astype(jnp.float32)
        numerator, denominator = mine * own_value[s], mine
        for t in range(tps):
            scale = jnp.exp(parts[t, 1, s] - top)
            numerator = numerator + parts[t, 0, s] * scale
            denominator = denominator + parts[t, 2, s] * scale
        rotated[s] = numerator / denominator

    for j in range(HQ):
        row = (j // group) * PAD + j % group
        attended[:, j * HD : (j + 1) * HD] = rotated[:, row, :].astype(attended.dtype)

    @pl.loop(0, widths[1] // tile)
    def _(i):
        at = pl.ds(pl.multiple_of(i * tile, tile), tile)
        under = pl.ds(pl.multiple_of(widths[0] + i * tile, tile), tile)
        decoded[:, at] = jnp.dot(
            attended[...], weights[:, under], preferred_element_type=jnp.float32
        ).astype(decoded.dtype)

    sent(bytes_of(tps - 1), local.at[5])
    sent(joined.at[pl.ds(0, tps - 1)], local.at[0])
    sent(parts.at[pl.ds(0, tps - 1)], local.at[1])
    settle_twin((planes - 1) * block, 0)
    settle_next(0)
    settle_next(planes - 1)
    at_end = (plane == 0) | (plane == planes - 1)
    relay(planes - 1)

    @pl.when((core == 1) & (plane == planes - 1))
    def _():
        take_tails(0)

    @pl.when((core == 1) & (plane == 0))
    def _():
        take_tails(planes - 1)

    @pl.when(at_end)
    def _():
        settle_twin(block - tail, 1)

    @pl.when(at_end & (core == 0))
    def _():
        landed(out_rows(2 * tail), t_recv.at[len(tails)])

    for p in range(1, planes - 1):
        settle_next(p)

    @pl.when((core == 1) & at_end)
    def _():
        sent(out_rows(2 * tail - 16), local.at[6])

    @pl.when((core == 1) & ((plane == 1) | (plane == planes - 2)))
    def _():
        sent(out_rows(2 * tail + 16), local.at[6])


def flush_kernel(decoded, qkv, out, decoded_to, qkv_to, out_to, sems):
    pairs = ((decoded, decoded_to), (qkv, qkv_to), (out, out_to))
    for i, (source, target) in enumerate(pairs):
        cuts = max(c for c in range(1, CUTS + 1) if c == 1 or source.shape[0] % (16 * c) == 0)
        rows = source.shape[0] // cuts
        for j in range(cuts):
            at = pl.ds(j * rows, rows)
            pltpu.make_async_copy(source.at[at], target.at[at], sems.at[i]).start()
    for i, (source, target) in enumerate(pairs):
        pltpu.make_async_copy(source, target, sems.at[i]).wait()


def flush(*arrays):
    return pl.pallas_call(
        flush_kernel,
        out_shape=[jax.ShapeDtypeStruct(x.shape, x.dtype) for x in arrays],
        in_specs=[pl.BlockSpec(memory_space=pltpu.VMEM)] * 3,
        out_specs=[pl.BlockSpec(memory_space=pltpu.HBM)] * 3,
        scratch_shapes=[pltpu.SemaphoreType.DMA((3,))],
        compiler_params=pltpu.CompilerParams(vmem_limit_bytes=2**20),
    )(*arrays)


def fused(mesh, hidden, lengths, old_qkv, old_out, keys, values, new_qkv, new_out):
    reps, tps = mesh.shape["rep"], mesh.shape["tp"]
    planes = reps // 2
    seqs = keys.shape[0]
    rows = new_qkv.shape[0]
    widths = (new_qkv.shape[1] // tps, new_out.shape[1] // tps)
    half = HD // 2
    frequency = ROPE_BASE ** (-2.0 * np.arange(half) / (2 * half))
    frequency = jnp.asarray(np.concatenate([frequency, frequency])[None], jnp.float32)

    sem = pltpu.SemaphoreType.DMA
    whole, anywhere = pl.BlockSpec(memory_space=pltpu.VMEM), pl.BlockSpec(memory_space=pl.ANY)
    in_hbm = pl.BlockSpec(memory_space=pltpu.HBM)
    f32, bf16 = jnp.float32, jnp.bfloat16
    padded = KVH * PAD
    landed = 2 * rows * reps * tps * sum(widths)
    scratch = [sem((tps - 1, 2)), sem((2,)), sem((planes - 1, tps // 2)), sem((2,)), sem((2,))]
    scratch += [sem((5,)), sem((4,)), sem((7,)), pltpu.SemaphoreType.REGULAR((2,))]
    scratch += [pltpu.VMEM((rows, new_qkv.shape[1] + new_out.shape[1]), bf16)]
    scratch += [pltpu.VMEM((DETOUR, widths[1]), bf16)]
    scratch += [pltpu.VMEM((old_qkv.shape[0], sum(widths)), bf16), pltpu.VMEM((2, *keys.shape), bf16)]
    scratch += [
        pltpu.VMEM((tps, seqs, widths[0]), bf16),
        pltpu.VMEM((seqs, padded, HD), f32),
        pltpu.VMEM((seqs, padded, HD), f32),
        pltpu.VMEM((seqs, padded, HD), f32),
        pltpu.VMEM((tps, 3, seqs, padded, HD), f32),
        pltpu.VMEM((seqs, HQ * HD), bf16),
        pltpu.VMEM((seqs, HD), f32),
        pltpu.VMEM((seqs, HD), f32),
        pltpu.VMEM(hidden.shape, hidden.dtype),
        pltpu.VMEM(frequency.shape, frequency.dtype),
        pltpu.SMEM(lengths.shape, lengths.dtype),
    ]
    return pl.pallas_call(
        functools.partial(step_kernel, planes, tps),
        out_shape=[pltpu.VMEM((seqs, widths[1]), bf16)]
        + [pltpu.VMEM((rows * reps * tps, width), bf16) for width in widths],
        in_specs=[in_hbm] * 9,
        out_specs=[whole] + [anywhere] * 2,
        scratch_shapes=scratch,
        compiler_params=pltpu.CompilerParams(
            collective_id=0, has_side_effects=True, vmem_limit_bytes=VMEM_BYTES - landed - SLACK
        ),
    )(hidden, lengths, frequency, old_qkv, old_out, keys, values, new_qkv, new_out)


def solution(mesh):
    in_specs = (
        P("rep", None),
        P("rep"),
        P(None, "tp"),
        P(None, "tp"),
        P("rep", "tp", None),
        P("rep", "tp", None),
        P(("rep", "tp"), None),
        P(("rep", "tp"), None),
    )
    out_specs = (P("rep", "tp"), P(None, "tp"), P(None, "tp"))

    def step(*args):
        reps, tps = mesh.shape["rep"], mesh.shape["tp"]
        widths = [x.shape[1] // tps for x in args[6:]]
        rows = args[6].shape[0]
        tiled = rows % 16 == 0 and all(width % 128 == 0 for width in widths)
        tiled = tiled and rows > max(TAIL * 8, DETOUR) and rows * tps * sum(widths) % widths[1] == 0
        tiled = tiled and args[2].shape[0] == args[3].shape[0]
        if reps % 4 or reps < 6 or tps != 4 or not tiled:
            return (per_device(*args[:6]), *native_move(*args[6:]))
        return tuple(flush(*fused(mesh, *args)))

    return jax.shard_map(
        step, mesh=mesh, in_specs=in_specs, out_specs=out_specs, check_vma=False
    )
```

```python
import functools

import jax
import jax.numpy as jnp
import numpy as np
from jax import lax
from jax.experimental import pallas as pl
from jax.experimental.pallas import tpu as pltpu
from jax.sharding import PartitionSpec as P

HQ = 28
KVH = 4
HD = 128
PAD = 8
CUTS = 56
TAIL = 4
DETOUR = 16
VMEM_BYTES = 67043328
SLACK = 600000
MESH = pl.DeviceIdType.MESH


ROPE_BASE = 1000000.0


def rotate(vectors, positions):
    half_dim = vectors.shape[-1] // 2
    frequency = ROPE_BASE ** (-2.0 * jnp.arange(half_dim, dtype=jnp.float32) / (2 * half_dim))
    angles = positions.astype(jnp.float32)[:, None, None] * frequency
    first_half = vectors[..., :half_dim]
    second_half = vectors[..., half_dim:]
    return jnp.concatenate(
        [
            first_half * jnp.cos(angles) - second_half * jnp.sin(angles),
            second_half * jnp.cos(angles) + first_half * jnp.sin(angles),
        ],
        axis=-1,
    )


def per_device(hidden_state, lengths, old_qkv, old_out, cache_keys, cache_values):
    seq_count = hidden_state.shape[0]
    local_joined = jnp.dot(hidden_state, old_qkv, preferred_element_type=jnp.float32).astype(
        jnp.bfloat16
    )
    joined_rows = lax.all_gather(local_joined, "tp", axis=1, tiled=True)
    q_width = HQ * HD
    k_width = KVH * HD
    group_size = HQ // KVH
    queries = rotate(
        joined_rows[:, :q_width].astype(jnp.float32).reshape(seq_count, HQ, HD), lengths
    ).astype(jnp.bfloat16)
    own_keys = rotate(
        joined_rows[:, q_width : q_width + k_width].astype(jnp.float32).reshape(seq_count, KVH, HD),
        lengths,
    ).astype(jnp.bfloat16)
    own_values = joined_rows[:, q_width + k_width :].reshape(seq_count, KVH, HD)
    inv_root = 1.0 / jnp.sqrt(jnp.float32(HD))
    cache_rows = cache_keys.shape[1]
    grouped = queries.reshape(seq_count, KVH, group_size, HD)
    key_blocks = cache_keys.reshape(seq_count, cache_rows, KVH, HD)
    value_blocks = cache_values.reshape(seq_count, cache_rows, KVH, HD)
    scores = (
        jnp.einsum("skgd,stkd->skgt", grouped, key_blocks, preferred_element_type=jnp.float32)
        * inv_root
    )
    positions = lax.axis_index("tp") * cache_rows + jnp.arange(cache_rows, dtype=jnp.int32)
    live_mask = (positions[None, :] < lengths[:, None])[:, None, None, :]
    scores = jnp.where(live_mask, scores, jnp.float32(-1e30))
    own_score = (
        jnp.sum(grouped.astype(jnp.float32) * own_keys.astype(jnp.float32)[:, :, None, :], axis=-1)
        * inv_root
    )
    local_top = jnp.maximum(jnp.max(scores, axis=-1), own_score)
    top_score = lax.pmax(local_top, "tp")
    weights = jnp.where(live_mask, jnp.exp(scores - top_score[..., None]), jnp.float32(0.0)).astype(
        jnp.bfloat16
    )
    numer_part = jnp.einsum(
        "skgt,stkd->skgd", weights, value_blocks, preferred_element_type=jnp.float32
    )
    denom_part = jnp.sum(weights.astype(jnp.float32), axis=-1)
    numerator, denominator = lax.psum((numer_part, denom_part), "tp")
    own_weight = lax.optimization_barrier(
        jnp.exp(own_score - top_score).astype(jnp.bfloat16)
    ).astype(jnp.float32)
    numerator = numerator + own_weight[..., None] * own_values.astype(jnp.float32)[:, :, None, :]
    denominator = denominator + own_weight
    attended = (numerator / denominator[..., None]).reshape(seq_count, q_width).astype(jnp.bfloat16)
    decoded = jnp.dot(attended, old_out, preferred_element_type=jnp.float32).astype(jnp.bfloat16)
    return decoded


def native_move(new_qkv, new_out):
    def move(block):
        piece = lax.all_to_all(block, "tp", split_axis=1, concat_axis=0, tiled=True)
        return lax.all_gather(piece, "rep", axis=0, tiled=True)

    return move(new_qkv), move(new_out)


def flip(index, bits, size):
    out = index
    bit = 1
    while bit < size:
        if (bits // bit) % 2:
            out = out + bit - 2 * bit * ((index // bit) % 2)
        bit *= 2
    return out


def step_kernel(
    planes, tps,
    hidden_in, lengths_in, frequency_in, old_qkv, old_out, keys, values, new_qkv, new_out,
    decoded, qkv_full, out_full,
    a_recv, z_send, z_recv, s_send, s_recv, t_recv, x_recv, local, met,
    stage, detour,
    weights, caches, joined, rotated, own_score, own_value, parts, attended,
    cosine, sine, hidden, frequency, lengths,
):
    rep, tp = lax.axis_index("rep"), lax.axis_index("tp")
    plane, core = rep // 2, rep % 2
    rows = new_qkv.shape[0]
    fulls = (qkv_full, out_full)
    widths = (qkv_full.shape[1], out_full.shape[1])
    bases = (0, new_qkv.shape[1])
    up = (jnp.minimum(plane + 1, planes - 1) * 2 + core, tp)
    down = (jnp.maximum(plane - 1, 0) * 2 + core, tp)
    twin = (plane * 2 + 1 - core, tp)
    peers = [(rep, flip(tp, k, tps)) for k in range(1, tps)]
    near = [k for k in range(1, tps) if k & (k - 1) == 0]
    far = [k for k in range(1, tps) if k & (k - 1)]
    can_up, can_down = plane < planes - 1, plane > 0

    half = tps // 2

    def at_rows(source_plane, source_core, first, count, w):
        start = ((source_plane * 2 + source_core) * tps) * rows + first
        return fulls[w].at[pl.ds(pl.multiple_of(start, 16), count)]

    def piece_rows(source_plane, source_core, k, w):
        return at_rows(source_plane, source_core, flip(tp, k, tps) * rows, rows, w)

    mine = [
        pltpu.make_async_copy(
            source.at[:, pl.ds(pl.multiple_of(tp * widths[w], 128), widths[w])],
            piece_rows(plane, core, 0, w), local.at[w],
        )
        for w, source in enumerate((new_qkv, new_out))
    ]
    staged = [
        pltpu.make_async_copy(
            source, stage.at[:, pl.ds(bases[w], source.shape[1])], local.at[2]
        )
        for w, source in enumerate((new_qkv, new_out))
    ]
    barrier = pltpu.get_barrier_semaphore()
    beside = [twin] + [peers[k - 1] for k in near]

    def tell(semaphore, device):
        pl.semaphore_signal(semaphore, inc=1, device_id=device, device_id_type=MESH)

    @pl.when(can_up)
    def _():
        tell(barrier, up)

    @pl.when(can_down & (plane != 2))
    def _():
        tell(barrier, down)

    @pl.when(plane != 1)
    def _():
        for device in beside:
            tell(barrier, device)
        for copy in mine + staged:
            copy.start()

    small = [
        pltpu.make_async_copy(source, target, local.at[i])
        for i, (source, target) in enumerate(
            ((hidden_in, hidden), (frequency_in, frequency), (lengths_in, lengths))
        )
    ]

    @pl.when(plane == 1)
    def _():
        pl.semaphore_wait(barrier, 1)

    @pl.when((plane != 1) & can_up & can_down)
    def _():
        pl.semaphore_wait(barrier, len(beside) + 2)

    @pl.when(jnp.logical_not(can_up & can_down))
    def _():
        pl.semaphore_wait(barrier, len(beside) + 1)

    def remote(source, target, send, recv, device):
        return pltpu.make_async_remote_copy(
            src_ref=source, dst_ref=target, send_sem=send, recv_sem=recv,
            device_id=device, device_id_type=MESH,
        )

    def sent(ref, sem):
        remote(ref, ref, sem, sem, twin).wait_send()

    def landed(ref, sem):
        remote(ref, ref, sem, sem, twin).wait_recv()

    def pair_first(h):
        return (flip(tp, 2 * h, tps) // 2) * 2 * rows

    tail = TAIL * 16
    tails = [(1, first, count) for first, count in ((2 * rows - tail, tail - 16), (2 * rows - 16, 16))]
    tails = [(c, part) for part in tails for c in (1, 0)]

    def parts_of(h, last):
        if last and h == half - 1:
            first = 2 * rows - 2 * tail
            return [(0, 0, 2 * rows, 0), (1, 0, first, 1), (1, first, tail, 2)]
        return [(w, 0, 2 * rows, 0) for w in range(2)]

    def part_rows(source_plane, source_core, h, part):
        w, first, count = part[:3]
        return at_rows(source_plane, source_core, pair_first(h) + first, count, w)

    def part_sem(index, h, part):
        return x_recv.at[(part[3] - 1) * 4] if part[3] else z_recv.at[index, h]

    def bytes_of(parts):
        return stage.at[:, pl.ds(0, stage.shape[1] // tps * parts)]

    def out_rows(count):
        return out_full.at[pl.ds(0, count)]

    def send_tails(source_plane, device):
        for i, (c, part) in enumerate(tails):
            ref = part_rows(source_plane, c, half - 1, part)
            if i == len(tails) - 1:
                other = (device[0] - 1, tp)
                remote(ref, ref, local.at[6], t_recv.at[len(tails)], other).start()
            remote(ref, ref, local.at[6], t_recv.at[i], device).start()

    def take_tails(source_plane):
        for i, (c, part) in enumerate(tails):
            ref = part_rows(source_plane, c, half - 1, part)
            landed(ref, t_recv.at[i])
            if i < len(tails) - 1:
                remote(ref, ref, local.at[6], t_recv.at[len(tails)], twin).start()

    def column(w, t):
        start = bases[w] + t * widths[w]
        return stage.at[:, pl.ds(pl.multiple_of(start, 128), widths[w])]

    def in_plane(k, w):
        remote(
            column(w, flip(tp, k, tps)), piece_rows(plane, core, 0, w),
            local.at[5], a_recv.at[k - 1, w], peers[k - 1],
        ).start()

    def own_up(k, w):
        ref = piece_rows(plane, core, k, w)

        @pl.when(can_up)
        def _():
            remote(ref, ref, z_send.at[0], z_recv.at[plane, k // 2], up).start()

    def own_down(k, w):
        ref = piece_rows(plane, core, k, w)

        def send(ref):
            remote(ref, ref, z_send.at[1], z_recv.at[plane - 1, k // 2], down).start()

        if w and k:
            short = detoured & (core == (k + 1) % 2)

            @pl.when(short)
            def _():
                send(at_rows(plane, core, flip(tp, k, tps) * rows, rows - DETOUR, w))

            @pl.when(can_down & jnp.logical_not(short))
            def _():
                send(ref)

        else:

            @pl.when(can_down)
            def _():
                send(ref)

    def own_twin(k, w):
        ref = piece_rows(plane, core, k, w)
        remote(ref, ref, s_send.at[0], s_recv.at[0], twin).start()

    detoured = (plane == 1) & (tp == 0)
    carries = (tp != 0) & (core == (tp + 1) % 2)

    def detour_down():
        @pl.when((plane == 1) & carries)
        def _():
            source = stage.at[pl.ds(rows - DETOUR, DETOUR), pl.ds(bases[1], widths[1])]
            remote(source, detour, local.at[6], x_recv.at[1], down).start()

    def detour_across():
        @pl.when((plane == 0) & carries)
        def _():
            landed(detour, x_recv.at[1])
            target = at_rows(1, core, tp * rows + rows - DETOUR, DETOUR, 1)
            remote(detour, target, local.at[6], z_recv.at[0, tp // 2], (rep, jnp.int32(0))).start()

    def take(source_plane, index, h, single, parts, far, can, device, way, onward):
        if single:
            (part,) = parts
            landed(part_rows(source_plane, core, h, part), part_sem(index, h, part))
        else:
            landed(bytes_of(2), z_recv.at[index, h])
        if onward:

            @pl.when(can)
            def _():
                for part in onward:
                    ref = part_rows(source_plane, core, h, part)
                    sem = part_sem(source_plane - way, h, part)
                    remote(ref, ref, z_send.at[way], sem, device).start()

        for part in parts:
            ref = part_rows(source_plane, core, h, part)
            remote(ref, ref, s_send.at[far], s_recv.at[far], twin).start()

    def farthest(source_plane):
        other = jnp.where(plane < planes // 2, planes - 1, 0)
        return jnp.where(source_plane == other, 1, 0)

    def relay(d):
        ends = d == planes - 1
        for h in range(half):
            cuts = parts_of(h, ends)
            onward = [] if ends else parts_of(h, d == planes - 2)
            single = ends and h == half - 1
            for parts in [[part] for part in cuts] if single else [cuts]:

                @pl.when(plane >= d)
                def _():
                    s = plane - d
                    take(s, s, h, single, parts, farthest(s), can_up, up, 0, onward)

                @pl.when(plane + d < planes)
                def _():
                    s = plane + d
                    take(s, s - 1, h, single, parts, farthest(s), can_down, down, 1, onward)

    block = rows * tps * sum(widths) // widths[1]

    def settle_twin(count, far):
        landed(out_rows(count), s_recv.at[far])
        sent(out_rows(count), s_send.at[far])

    def settle_next(p):
        @pl.when(plane == p)
        def _():
            for way, count in ((0, p + 1), (1, planes - p)):
                if p == (planes - 1, 0)[way]:
                    continue
                total = count * block - (tail if p == (planes - 2, 1)[way] else 0)
                if p != 1 or way == 0:
                    sent(out_rows(total), z_send.at[way])
                    continue

                @pl.when(tp != 0)
                def _():
                    sent(out_rows(total), z_send.at[way])

                for c in range(2):
                    cut = DETOUR * sum((k + 1) % 2 == c for k in range(1, tps))

                    @pl.when((tp == 0) & (core == c))
                    def _():
                        sent(out_rows(total - cut), z_send.at[way])

    @pl.when(plane == 1)
    def _():
        for w, source in enumerate((new_qkv, new_out)):
            columns = pl.ds(pl.multiple_of(tp * widths[w], 128), widths[w])
            remote(
                source.at[:, columns], piece_rows(plane, core, 0, w),
                z_send.at[1], z_recv.at[plane - 1, 0], down,
            ).start()
        for copy in mine + staged:
            copy.start()

    for w in range(2):
        mine[w].wait()

        @pl.when(plane != 1)
        def _():
            own_down(0, w)

    def open_plane():
        pltpu.make_async_copy(stage, stage, local.at[2]).wait()
        for w in (1, 0):
            for k in near:
                in_plane(k, w)
        for w in range(2):
            own_twin(0, w)

    @pl.when(plane == 0)
    def _():
        for device in beside:
            tell(met.at[0], device)

    @pl.when(plane == 2)
    def _():
        tell(met.at[1], down)

    @pl.when(plane != 1)
    def _():
        for w in range(2):
            own_up(0, w)
        open_plane()

    @pl.when(plane == 0)
    def _():
        pl.semaphore_wait(met.at[0], len(beside))
        tell(met.at[0], up)

    @pl.when(plane == 1)
    def _():
        pl.semaphore_wait(met.at[0], 1)
        open_plane()
        detour_down()
        pl.semaphore_wait(met.at[1], 1)
        for w in range(2):
            own_up(0, w)

    held = [caches.at[i] for i in range(2)]
    loads = [
        pltpu.make_async_copy(source, target, local.at[3 + i])
        for sources, targets, i in (
            ((old_qkv, old_out), [weights.at[:, pl.ds(sum(widths[:w]), widths[w])] for w in range(2)], 0),
            ((keys, values), held, 1),
        )
        for source, target in zip(sources, targets)
    ]
    for copy in loads + small:
        copy.start()
    arrivals = [(k, w) for w in (1, 0) for k in near] + [(k, w) for k in far for w in (1, 0)]
    for k, w in arrivals:
        landed(piece_rows(plane, core, k, w), a_recv.at[k - 1, w])
        own_down(k, w)
        own_up(k, w)
        own_twin(k, w)
        if (k, w) == arrivals[0]:
            for j in far:
                for v in (1, 0):
                    in_plane(j, v)

    detour_across()
    for copy in small:
        copy.wait()
    seqs = hidden.shape[0]
    lane = lax.broadcasted_iota(jnp.int32, (1, HD), 1)
    for s in range(seqs):
        angles = lengths[s].astype(jnp.float32) * frequency[...]
        cosine[s : s + 1, :] = jnp.cos(angles)
        sine[s : s + 1, :] = jnp.where(lane < HD // 2, -jnp.sin(angles), jnp.sin(angles))
    tile = 128
    pltpu.make_async_copy(weights, weights, local.at[3]).wait()
    pltpu.make_async_copy(caches, caches, local.at[4]).wait()

    @pl.loop(0, widths[0] // tile)
    def _(i):
        at = pl.ds(pl.multiple_of(i * tile, tile), tile)
        joined[tp, :, at] = jnp.dot(
            hidden[...], weights[:, at], preferred_element_type=jnp.float32
        ).astype(joined.dtype)

    def send_all(ref, send, recv):
        for k in range(1, tps):
            remote(ref.at[tp], ref.at[tp], send, recv, peers[k - 1]).start()

    send_all(joined, local.at[0], x_recv.at[2])

    relay(1)

    landed(joined.at[pl.ds(0, tps - 1)], x_recv.at[2])

    group = HQ // KVH
    positions = caches.shape[2]
    per_slot = joined.shape[2] // HD
    inv_root = 1.0 / jnp.sqrt(jnp.float32(HD))

    def head(j):
        at = (j % per_slot) * HD
        return joined[j // per_slot, :, at : at + HD].astype(jnp.float32)

    def turn(v):
        swapped = jnp.concatenate([v[:, HD // 2 :], v[:, : HD // 2]], axis=1)
        return (v * cosine[...] + swapped * sine[...]).astype(jnp.bfloat16).astype(jnp.float32)

    rotated[...] = jnp.zeros_like(rotated)
    own_score[...] = jnp.zeros_like(own_score)
    own_value[...] = jnp.zeros_like(own_value)
    for kv in range(KVH):
        own_key = turn(head(HQ + kv))
        new_value = head(HQ + KVH + kv)
        for g in range(group):
            query = turn(head(kv * group + g))
            rotated[:, kv * PAD + g, :] = query
            score = jnp.sum(query * own_key, axis=1, keepdims=True) * inv_root
            own_score[:, kv * PAD + g, :] = jnp.broadcast_to(score, (seqs, HD))
            own_value[:, kv * PAD + g, :] = new_value

    @pl.loop(0, seqs)
    def _(s):
        place = lax.broadcasted_iota(jnp.int32, (1, positions), 1) + tp * positions
        is_live = place < lengths[s]
        for kv in range(KVH):
            at = slice(kv * HD, (kv + 1) * HD)
            lanes = slice(kv * PAD, (kv + 1) * PAD)
            query = rotated[s, lanes, :].astype(jnp.bfloat16)
            scores = lax.dot_general(
                query, caches[0, s, :, at], (((1,), (1,)), ((), ())),
                preferred_element_type=jnp.float32,
            ) * inv_root
            scores = jnp.where(is_live, scores, jnp.float32(-1e30))
            top = jnp.max(scores, axis=1, keepdims=True)
            shares = jnp.where(is_live, jnp.exp(scores - top), 0.0).astype(jnp.bfloat16)
            total = jnp.sum(shares.astype(jnp.float32), axis=1, keepdims=True)
            parts[tp, 0, s, lanes, :] = jnp.dot(
                shares, caches[1, s, :, at], preferred_element_type=jnp.float32
            )
            parts[tp, 1, s, lanes, :] = jnp.broadcast_to(top, (PAD, HD))
            parts[tp, 2, s, lanes, :] = jnp.broadcast_to(total, (PAD, HD))

    send_all(parts, local.at[1], x_recv.at[3])

    for d in range(2, planes - 1):
        relay(d)
    @pl.when((plane < 2) & carries)
    def _():
        sent(detour, local.at[6])

    @pl.when((plane == 1) | (plane == planes - 2))
    def _():
        settle_twin(block, 1)

    @pl.when((core == 1) & (plane == planes - 2))
    def _():
        send_tails(0, up)

    @pl.when((core == 1) & (plane == 1))
    def _():
        send_tails(planes - 1, down)


    landed(parts.at[pl.ds(0, tps - 1)], x_recv.at[3])

    @pl.loop(0, seqs)
    def _(s):
        mine = own_score[s]
        top = mine
        for t in range(tps):
            top = jnp.maximum(top, parts[t, 1, s])
        mine = jnp.exp(mine - top).astype(jnp.bfloat16).astype(jnp.float32)
        numerator, denominator = mine * own_value[s], mine
        for t in range(tps):
            scale = jnp.exp(parts[t, 1, s] - top)
            numerator = numerator + parts[t, 0, s] * scale
            denominator = denominator + parts[t, 2, s] * scale
        rotated[s] = numerator / denominator

    for j in range(HQ):
        row = (j // group) * PAD + j % group
        attended[:, j * HD : (j + 1) * HD] = rotated[:, row, :].astype(attended.dtype)

    @pl.loop(0, widths[1] // tile)
    def _(i):
        at = pl.ds(pl.multiple_of(i * tile, tile), tile)
        under = pl.ds(pl.multiple_of(widths[0] + i * tile, tile), tile)
        decoded[:, at] = jnp.dot(
            attended[...], weights[:, under], preferred_element_type=jnp.float32
        ).astype(decoded.dtype)

    sent(bytes_of(tps - 1), local.at[5])
    sent(joined.at[pl.ds(0, tps - 1)], local.at[0])
    sent(parts.at[pl.ds(0, tps - 1)], local.at[1])
    settle_twin((planes - 1) * block, 0)
    settle_next(0)
    settle_next(planes - 1)
    at_end = (plane == 0) | (plane == planes - 1)
    relay(planes - 1)

    @pl.when((core == 1) & (plane == planes - 1))
    def _():
        take_tails(0)

    @pl.when((core == 1) & (plane == 0))
    def _():
        take_tails(planes - 1)

    @pl.when(at_end)
    def _():
        settle_twin(block - tail, 1)

    @pl.when(at_end & (core == 0))
    def _():
        landed(out_rows(2 * tail), t_recv.at[len(tails)])

    for p in range(1, planes - 1):
        settle_next(p)

    @pl.when((core == 1) & at_end)
    def _():
        sent(out_rows(2 * tail - 16), local.at[6])

    @pl.when((core == 1) & ((plane == 1) | (plane == planes - 2)))
    def _():
        sent(out_rows(2 * tail + 16), local.at[6])


def flush_kernel(decoded, qkv, out, decoded_to, qkv_to, out_to, sems):
    pairs = ((decoded, decoded_to), (qkv, qkv_to), (out, out_to))
    for i, (source, target) in enumerate(pairs):
        cuts = max(c for c in range(1, CUTS + 1) if c == 1 or source.shape[0] % (16 * c) == 0)
        rows = source.shape[0] // cuts
        for j in range(cuts):
            at = pl.ds(j * rows, rows)
            pltpu.make_async_copy(source.at[at], target.at[at], sems.at[i]).start()
    for i, (source, target) in enumerate(pairs):
        pltpu.make_async_copy(source, target, sems.at[i]).wait()


def flush(*arrays):
    return pl.pallas_call(
        flush_kernel,
        out_shape=[jax.ShapeDtypeStruct(x.shape, x.dtype) for x in arrays],
        in_specs=[pl.BlockSpec(memory_space=pltpu.VMEM)] * 3,
        out_specs=[pl.BlockSpec(memory_space=pltpu.HBM)] * 3,
        scratch_shapes=[pltpu.SemaphoreType.DMA((3,))],
        compiler_params=pltpu.CompilerParams(vmem_limit_bytes=2**20),
    )(*arrays)


def fused(mesh, hidden, lengths, old_qkv, old_out, keys, values, new_qkv, new_out):
    reps, tps = mesh.shape["rep"], mesh.shape["tp"]
    planes = reps // 2
    seqs = keys.shape[0]
    rows = new_qkv.shape[0]
    widths = (new_qkv.shape[1] // tps, new_out.shape[1] // tps)
    half = HD // 2
    frequency = ROPE_BASE ** (-2.0 * np.arange(half) / (2 * half))
    frequency = jnp.asarray(np.concatenate([frequency, frequency])[None], jnp.float32)

    sem = pltpu.SemaphoreType.DMA
    whole, anywhere = pl.BlockSpec(memory_space=pltpu.VMEM), pl.BlockSpec(memory_space=pl.ANY)
    in_hbm = pl.BlockSpec(memory_space=pltpu.HBM)
    f32, bf16 = jnp.float32, jnp.bfloat16
    padded = KVH * PAD
    landed = 2 * rows * reps * tps * sum(widths)
    scratch = [sem((tps - 1, 2)), sem((2,)), sem((planes - 1, tps // 2)), sem((2,)), sem((2,))]
    scratch += [sem((5,)), sem((5,)), sem((7,)), pltpu.SemaphoreType.REGULAR((2,))]
    scratch += [pltpu.VMEM((rows, new_qkv.shape[1] + new_out.shape[1]), bf16)]
    scratch += [pltpu.VMEM((DETOUR, widths[1]), bf16)]
    scratch += [pltpu.VMEM((old_qkv.shape[0], sum(widths)), bf16), pltpu.VMEM((2, *keys.shape), bf16)]
    scratch += [
        pltpu.VMEM((tps, seqs, widths[0]), bf16),
        pltpu.VMEM((seqs, padded, HD), f32),
        pltpu.VMEM((seqs, padded, HD), f32),
        pltpu.VMEM((seqs, padded, HD), f32),
        pltpu.VMEM((tps, 3, seqs, padded, HD), f32),
        pltpu.VMEM((seqs, HQ * HD), bf16),
        pltpu.VMEM((seqs, HD), f32),
        pltpu.VMEM((seqs, HD), f32),
        pltpu.VMEM(hidden.shape, hidden.dtype),
        pltpu.VMEM(frequency.shape, frequency.dtype),
        pltpu.SMEM(lengths.shape, lengths.dtype),
    ]
    return pl.pallas_call(
        functools.partial(step_kernel, planes, tps),
        out_shape=[pltpu.VMEM((seqs, widths[1]), bf16)]
        + [pltpu.VMEM((rows * reps * tps, width), bf16) for width in widths],
        in_specs=[in_hbm] * 9,
        out_specs=[whole] + [anywhere] * 2,
        scratch_shapes=scratch,
        compiler_params=pltpu.CompilerParams(
            collective_id=0, has_side_effects=True, vmem_limit_bytes=VMEM_BYTES - landed - SLACK
        ),
    )(hidden, lengths, frequency, old_qkv, old_out, keys, values, new_qkv, new_out)


def solution(mesh):
    in_specs = (
        P("rep", None),
        P("rep"),
        P(None, "tp"),
        P(None, "tp"),
        P("rep", "tp", None),
        P("rep", "tp", None),
        P(("rep", "tp"), None),
        P(("rep", "tp"), None),
    )
    out_specs = (P("rep", "tp"), P(None, "tp"), P(None, "tp"))

    def step(*args):
        reps, tps = mesh.shape["rep"], mesh.shape["tp"]
        widths = [x.shape[1] // tps for x in args[6:]]
        rows = args[6].shape[0]
        tiled = rows % 16 == 0 and all(width % 128 == 0 for width in widths)
        tiled = tiled and rows > max(TAIL * 16, DETOUR) and rows * tps * sum(widths) % widths[1] == 0
        tiled = tiled and args[2].shape[0] == args[3].shape[0]
        if reps % 4 or reps < 6 or tps != 4 or not tiled:
            return (per_device(*args[:6]), *native_move(*args[6:]))
        return tuple(flush(*fused(mesh, *args)))

    return jax.shard_map(
        step, mesh=mesh, in_specs=in_specs, out_specs=out_specs, check_vma=False
    )
```
